32 devices in a mesh: groups: 2 (over y), gx: 4 (over z), gy: 2 (over x), gz: 2 (over core).
Axes of the slice: x: 2, y: 2, z: 4, core: 2. Of those that a mesh axis runs over, the one named last changes fastest.
Arguments:
- coords: float32 [8, 8, 16, 3, 128], P(('groups', 'gx'), 'gy', 'gz'), parts along dimension 0, may hold values from 0 to 1.1
- charges: float32 [8, 8, 16, 128], P(('groups', 'gx'), 'gy', 'gz'), parts along dimension 0, may hold values from -2 to 2
- atom_types: int32 [8, 8, 16, 128], P(('groups', 'gx'), 'gy', 'gz'), parts along dimension 0, may hold values from 0 to 63
- counts: int32 [8, 8, 16], P(('groups', 'gx'), 'gy', 'gz'), parts along dimension 0, may hold values from 64 to 128
- c6_table: float32 [64, 64], replicated, may hold values from 0.0001 to 0.001
- c12_table: float32 [64, 64], replicated, may hold values from 1e-08 to 1e-07
Outputs:
- forces: float32 [8, 8, 16, 3, 128], P(('groups', 'gx'), 'gy', 'gz'), parts along dimension 0
- energy: float32 [2], P('groups'), parts along dimension 0
The draws below stay inside these ranges and needn't reach their ends.
There are 2 independent parts, one for each index of `groups`. The reference program is written for one: setup_inputs(seed, part) draws one part's arguments, and reference() takes and returns one part's arrays. A program takes and returns all parts, laid end to end along the dimension named above; an argument that names none is the same for every part. Nothing has to cross between parts.
All inputs are finite; a program needn't handle non-finite values.
Results may differ from the reference program's by a relative error of at most 0.0003.
Values sent between devices are 32-bit elements; how exact they have to be, the bound alone decides.
No kernel may reach another device: no remote copies, remote signals or barrier semaphores. Data moves between devices by JAX's collectives and lax.ppermute only.
A program may use at most 64 MiB of HBM per device.

```python
import math
import jax
import jax.numpy as jnp
from jax import lax

SLOTS = 128
TYPES = 64
NX = 4
NY = 8
NZ = 16


def set_ends(result, stream_key, low, top_value):
    index_at = [jax.random.randint(jax.random.fold_in(stream_key, axis), (), 0, length) for axis, length in enumerate(result.shape)]
    widest = result.shape.index(max(result.shape))
    beside = index_at[:widest] + [(index_at[widest] + 1) % result.shape[widest]] + index_at[widest + 1:]
    return result.at[tuple(index_at)].set(low).at[tuple(beside)].set(top_value)


def steps_of(key, extent, cuts, least, top_value):
    factor_of = 1.0
    for position, blocks in cuts:
        draws = jax.random.uniform(jax.random.fold_in(jax.random.fold_in(key, 6), position), (blocks,), jnp.float32, least / len(cuts), top_value / len(cuts))
        factor_of = factor_of * jnp.repeat(jnp.exp(draws), extent[position] // blocks).reshape((-1,) + (1,) * (len(extent) - 1 - position))
    return factor_of


def bell_draw(own_key, dims, scale, reach, split=(), kind=jnp.bfloat16):
    level = steps_of(own_key, dims, split, -0.22, 0.18) if split else 1.0
    result = jax.random.normal(own_key, dims, jnp.float32) * scale * level
    return jnp.minimum(jnp.maximum(result, -reach), reach).astype(kind)


def setup_inputs(seed: int = 0, part: int = 0) -> dict:
    streams_of = jax.random.split(jax.random.key(seed), 7)
    own_keys = jax.random.split(jax.random.fold_in(streams_of[6], part), 7)
    return {
        "coords": jnp.clip(1.1 * jax.random.uniform(own_keys[0], (NX, NY, NZ, 3, SLOTS), jnp.float32) ** steps_of(own_keys[0], (NX, NY, NZ, 3, SLOTS), ((0, 4), (1, 2), (2, 2)), -0.2, 0.2), 0.0, 1.1),
        "charges": bell_draw(own_keys[1], (NX, NY, NZ, SLOTS), 0.4, 2.0, ((0, 4), (1, 2), (2, 2)), jnp.float32),
        "atom_types": set_ends(jax.random.randint(own_keys[2], (NX, NY, NZ, SLOTS), 0, TYPES), jax.random.fold_in(own_keys[2], 1), 0, TYPES - 1).astype(jnp.int32),
        "counts": set_ends(jax.random.randint(own_keys[3], (NX, NY, NZ), SLOTS // 2, SLOTS + 1), jax.random.fold_in(own_keys[3], 1), SLOTS // 2, SLOTS).astype(jnp.int32),
        "c6_table": jnp.clip(jnp.exp(jax.random.uniform(streams_of[4], (TYPES, TYPES), jnp.float32, math.log(0.0001), math.log(0.001))), 0.0001, 0.001),
        "c12_table": jnp.clip(jnp.exp(jax.random.uniform(streams_of[5], (TYPES, TYPES), jnp.float32, math.log(9.99999993922529e-09), math.log(1.0000000116860974e-07))), 9.99999993922529e-09, 1.0000000116860974e-07),
    }


CELL_EDGE = 1.1
CUT_SQUARE = 1.0
SOFTEN = 0.09
ENERGY_UNIT = 0.1
CELL_PAIRS = ((0, 1), (0, 2), (0, 3), (0, 4), (0, 5), (0, 6), (0, 7), (1, 2), (1, 4), (2, 4), (1, 6), (2, 5), (4, 3))

def corner_bits(corner_index):
    return (corner_index >> 2 & 1, corner_index >> 1 & 1, corner_index & 1)

def pack_cells(coords, charges, atom_types, counts):
    slot_count = coords.shape[-1]
    occupied = (jnp.arange(slot_count, dtype=jnp.int32) < counts[..., None]).astype(jnp.float32)
    return jnp.concatenate([coords, charges[..., None, :], atom_types.astype(jnp.float32)[..., None, :], occupied[..., None, :]], axis=3)

def tile_terms(pack_a, pack_b, c6_sym, c12_sym, offset, pair_mask):
    type_ids = jnp.arange(c6_sym.shape[0]).astype(jnp.float32)
    type_hot_a = (pack_a[4][:, None] == type_ids[None, :]).astype(jnp.float32)
    type_hot_b = (pack_b[4][:, None] == type_ids[None, :]).astype(jnp.float32)
    c6_pair = jnp.dot(jnp.dot(type_hot_a, c6_sym, precision=lax.Precision.HIGHEST), type_hot_b.T, precision=lax.Precision.HIGHEST)
    c12_pair = jnp.dot(jnp.dot(type_hot_a, c12_sym, precision=lax.Precision.HIGHEST), type_hot_b.T, precision=lax.Precision.HIGHEST)
    charge_pair = pack_a[3][:, None] * pack_b[3][None, :]
    occupied_pair = pack_a[5][:, None] * pack_b[5][None, :] * pair_mask
    edge_inverse = 1.0 / (CUT_SQUARE + SOFTEN)
    edge_cube = edge_inverse ** 3

    def pair_energy(position_a, position_b):
        separation = position_b[:, None, :] - position_a[:, :, None] + offset[:, None, None]
        dist_square = lax.optimization_barrier(jnp.sum(separation * separation, axis=0))
        inverse = 1.0 / (dist_square + SOFTEN)
        inverse_cube = inverse * inverse * inverse
        coulomb = charge_pair * (jnp.sqrt(inverse) - edge_inverse ** 0.5)
        dispersion = c12_pair * (inverse_cube * inverse_cube - edge_cube * edge_cube) - c6_pair * (inverse_cube - edge_cube)
        cutoff_taper = jnp.maximum(1.0 - dist_square / CUT_SQUARE, 0.0)
        return ENERGY_UNIT * jnp.sum((coulomb + dispersion) * cutoff_taper * cutoff_taper * occupied_pair)
    energy, (grad_a, grad_b) = jax.value_and_grad(pair_energy, argnums=(0, 1))(pack_a[:3], pack_b[:3])
    return (energy, -grad_a, -grad_b)

def cell_batch(packs_a, packs_b, c6_sym, c12_sym, offset, pair_mask):

    def single(tiles):
        return tile_terms(tiles[0], tiles[1], c6_sym, c12_sym, offset, pair_mask)
    return lax.map(single, (packs_a, packs_b), batch_size=8)

def reference(coords, charges, atom_types, counts, c6_table, c12_table):
    c6_sym = 0.5 * (c6_table + c6_table.T)
    c12_sym = 0.5 * (c12_table + c12_table.T)
    packed = pack_cells(coords, charges, atom_types, counts)
    grid_shape = packed.shape[:3]
    slot_count = packed.shape[-1]
    upper_pairs = jnp.triu(jnp.ones((slot_count, slot_count), jnp.float32), 1)
    all_pairs = jnp.ones((slot_count, slot_count), jnp.float32)
    forces = jnp.zeros(grid_shape + (3, slot_count), jnp.float32)
    energy_sum = jnp.zeros((), jnp.float32)
    for source, target in ((0, 0),) + CELL_PAIRS:
        corner_a = corner_bits(source)
        corner_b = corner_bits(target)
        cells_a = jnp.roll(packed, (-corner_a[0], -corner_a[1], -corner_a[2]), axis=(0, 1, 2))
        cells_b = jnp.roll(packed, (-corner_b[0], -corner_b[1], -corner_b[2]), axis=(0, 1, 2))
        offset = jnp.array([(corner_b[k] - corner_a[k]) * CELL_EDGE for k in range(3)], jnp.float32)
        pair_mask = upper_pairs if source == target else all_pairs
        energies, force_a, force_b = cell_batch(cells_a.reshape((-1, 6, slot_count)), cells_b.reshape((-1, 6, slot_count)), c6_sym, c12_sym, offset, pair_mask)
        force_a = jnp.roll(force_a.reshape(grid_shape + (3, slot_count)), corner_a, axis=(0, 1, 2))
        force_b = jnp.roll(force_b.reshape(grid_shape + (3, slot_count)), corner_b, axis=(0, 1, 2))
        forces = forces + force_a + force_b
        energy_sum = energy_sum + jnp.sum(energies)
    return (forces, energy_sum.reshape(1))
```

```python
import jax
import jax.numpy as jnp
import numpy as np
from jax import lax
from jax.experimental import pallas as pl
from jax.experimental.pallas import tpu as pltpu
from jax.sharding import PartitionSpec as P

CELL_EDGE = 1.1
CUT_SQUARE = 1.0
SOFTEN = 0.09
ENERGY_UNIT = 0.1
EDGE_T = CUT_SQUARE + SOFTEN
K1 = EDGE_T**-0.5
K3 = EDGE_T**-3.0
K6 = EDGE_T**-6.0
OFFSETS = (
    (0, 0, 0),
    (0, 0, 1),
    (0, 1, 0),
    (0, 1, 1),
    (0, 1, -1),
) + tuple((1, oy, oz) for oy in (-1, 0, 1) for oz in (-1, 0, 1))
ROWS = 32


def shifted(block, axis, distance):
    devices = range(lax.axis_size(axis))
    route = [((i - distance) % len(devices), i) for i in devices]
    return lax.ppermute(block, axis, route)


def allowed(offset, at_low, at_high):
    if at_low:
        return offset >= 0
    if at_high:
        return offset < 0
    return True


def pair_kernel(counts_ref, feats_ref, table_ref, left_ref, forces_ref, fe, types, rows_a, fa, fb, eacc):
    ext_x, ext_y, ext_z = feats_ref.shape[:3]
    cells_x, cells_y, cells_z = ext_x - 1, ext_y - 1, ext_z - 1
    slots = feats_ref.shape[-1]
    row_id = lax.broadcasted_iota(jnp.int32, (8, slots), 0)
    eacc[...] = jnp.zeros_like(eacc)

    def place(ix, iy, iz):
        f = feats_ref[ix, iy, iz]
        shift = jnp.where(row_id == 0, ix, jnp.where(row_id == 1, iy, jnp.where(row_id == 2, iz, 0)))
        fe[ix, iy, iz] = f + shift.astype(jnp.float32) * CELL_EDGE
        types[ix, iy, iz] = f[4:5].astype(jnp.int32)
        fb[ix, iy, iz] = jnp.zeros(fb.shape[3:], jnp.float32)

    def place_plane(plane, _):
        ix = plane // ext_y
        iy = plane % ext_y
        for iz in range(ext_z):
            place(ix, iy, iz)
        return 0

    lax.fori_loop(0, ext_x * ext_y, place_plane, 0)

    lane_of = lax.broadcasted_iota(jnp.int32, (slots, slots), 1).astype(jnp.float32)
    f32, bf16 = jnp.float32, jnp.bfloat16

    def prepare(ix, iy, iz, slot):
        f = fe[ix, iy, iz]
        high = f.astype(bf16).astype(f32)
        mid = (f - high).astype(bf16).astype(f32)
        parts = jnp.concatenate([high, mid, f - high - mid], axis=0).T.astype(bf16)
        mine = jnp.dot(parts, left_ref[...], preferred_element_type=f32)
        hot = (mine[:, 4 * slots :] == lane_of).astype(f32).astype(bf16)
        looked = jnp.dot(jnp.concatenate([hot, hot], axis=1), table_ref[...], preferred_element_type=f32)
        for k in range(4):
            rows_a[slot, k] = mine[:, k * slots : (k + 1) * slots]
        for k in range(2):
            rows_a[slot, 4 + k] = looked[:, k * slots : (k + 1) * slots]

    def row_cell(ix, iy, iz, slot, offsets):
        count = counts_ref[ix, iy, iz]
        full = (count + (ROWS // 2 - 1)) // ROWS
        part = (count - full * ROWS + (ROWS - 1)) // ROWS

        def chunk(c, energy, rows):
            at = pl.multiple_of(c * ROWS, ROWS)
            here = pl.ds(at, rows)
            ax, ay, az, aq, a6, a12 = (rows_a[slot, k, here, :] for k in range(6))
            fx = fy = fz = None
            for ox, oy, oz in offsets:
                cell = (ix + ox, iy + oy, iz + oz)
                spread = lambda k: jnp.broadcast_to(fe[cell[0], cell[1], cell[2], k : k + 1, :], (rows, slots))
                dx = spread(0) - ax
                dy = spread(1) - ay
                dz = spread(2) - az
                qq = spread(3) * aq
                kind = jnp.broadcast_to(types[cell[0], cell[1], cell[2]], (rows, slots))
                c6, c12 = (
                    jnp.take_along_axis(t, kind, axis=1, mode="promise_in_bounds") for t in (a6, a12)
                )
                t = dx * dx + dy * dy + (dz * dz + SOFTEN)
                y = lax.rsqrt(t)
                v = y * y
                v3 = v * v * v
                p = qq * y
                h = c12 * v3
                m = h - c6
                gap = v3 - K3
                u = qq * (y - K1) + gap * m
                z = p + (6.0 * v3) * (m + c12 * gap)
                w = jnp.maximum(EDGE_T - t, 0.0)
                if (ox, oy, oz) == (0, 0, 0):
                    lane = lax.broadcasted_iota(jnp.int32, (rows, slots), 1)
                    row = lax.broadcasted_iota(jnp.int32, (rows, slots), 0) + at
                    w = jnp.where(lane > row, w, 0.0)
                s = w * ((w * v) * z + 4.0 * u)
                e = w * (w * u)
                for r in range(0, rows, 8):
                    energy = energy + e[r : r + 8]
                px, py, pz = s * dx, s * dy, s * dz
                for k, part in enumerate((px, py, pz)):
                    fold = part[0:8]
                    for r in range(8, rows, 8):
                        fold = fold + part[r : r + 8]
                    fb[cell[0], cell[1], cell[2], k] = fb[cell[0], cell[1], cell[2], k] + fold
                if fx is None:
                    fx, fy, fz = px, py, pz
                else:
                    fx, fy, fz = fx + px, fy + py, fz + pz
            for k, part in enumerate((fx, fy, fz)):
                fa[slot, k, here, :] = part
            return energy

        energy = lax.fori_loop(0, full, lambda c, e: chunk(c, e, ROWS), eacc[...])
        eacc[...] = lax.fori_loop(full, full + part, lambda c, e: chunk(c, e, ROWS // 2), energy)

    lane8 = lax.broadcasted_iota(jnp.int32, (slots, slots), 1)

    def finish(ix, iy, iz, slot):
        sums = [jnp.sum(fa[slot, k], axis=1, keepdims=True) for k in range(3)]
        packed = jnp.where(lane8 == 0, sums[0], jnp.where(lane8 == 1, sums[1], jnp.where(lane8 == 2, sums[2], 0.0)))
        forces_ref[ix, iy, iz] = -packed.T[:8]

    def row_line(ix, iy, low, high):
        fa[...] = jnp.zeros_like(fa)
        for iz in range(ext_z):
            prepare(ix, iy, iz, iz)

        def cells_at(iz, z_low, z_high):
            offsets = [
                o for o in OFFSETS if allowed(o[1], low, high) and allowed(o[2], z_low, z_high)
            ]
            row_cell(ix, iy, iz, iz, offsets)

        cells_at(0, True, False)

        def middle(iz, _):
            cells_at(iz, False, False)
            return 0

        lax.fori_loop(1, cells_z, middle, 0)
        cells_at(cells_z, False, True)
        for iz in range(ext_z):
            finish(ix, iy, iz, iz)

    def layer(ix, _):
        row_line(ix, 0, True, False)

        def middle(iy, _):
            row_line(ix, iy, False, False)
            return 0

        lax.fori_loop(1, cells_y, middle, 0)
        row_line(ix, cells_y, False, True)
        return 0

    lax.fori_loop(0, cells_x, layer, 0)

    energy_row = jnp.sum(eacc[...], axis=0, keepdims=True)

    def close(plane, _):
        ix = plane // ext_y
        iy = plane % ext_y
        for iz in range(ext_z):
            parts = [jnp.sum(fb[ix, iy, iz, k], axis=0, keepdims=True) for k in range(3)]
            total = jnp.concatenate(parts + [energy_row, jnp.zeros((4, slots), f32)], axis=0)
            held = jnp.where(ix < cells_x, forces_ref[ix, iy, iz], 0.0)
            forces_ref[ix, iy, iz] = held + total
        return 0

    lax.fori_loop(0, ext_x * ext_y, close, 0)


def pair_call(counts, feats, tables):
    ext = feats.shape[:3]
    slots = feats.shape[-1]
    f32 = jnp.float32
    left = np.zeros((24, 5 * slots), np.float32)
    for k in range(5):
        for n in range(3):
            left[8 * n + k, k * slots : (k + 1) * slots] = 1.0
    vmem = pl.BlockSpec(memory_space=pltpu.VMEM)
    return pl.pallas_call(
        pair_kernel,
        out_shape=jax.ShapeDtypeStruct(ext + (8, slots), f32),
        in_specs=[pl.BlockSpec(memory_space=pltpu.SMEM), vmem, vmem, vmem],
        out_specs=vmem,
        scratch_shapes=[
            pltpu.VMEM(ext + (8, slots), f32),
            pltpu.VMEM(ext + (1, slots), jnp.int32),
            pltpu.VMEM((ext[2], 6, slots, slots), f32),
            pltpu.VMEM((ext[2], 3, slots, slots), f32),
            pltpu.VMEM(ext + (3, 8, slots), f32),
            pltpu.VMEM((8, slots), f32),
        ],
        name="pair_forces",
    )(counts, feats, tables, jnp.asarray(left, jnp.bfloat16))


def make_tables(c6_table, c12_table, slots):
    c6 = (0.5 * ENERGY_UNIT) * (c6_table + c6_table.T)
    c12 = (0.5 * ENERGY_UNIT) * (c12_table + c12_table.T)
    more = slots - c6.shape[0]
    full = jnp.concatenate([jnp.pad(m, ((0, more), (0, more))) for m in (c6 - c12 * K3, c12)], axis=1)
    high = lax.reduce_precision(full, 8, 7)
    return jnp.concatenate([high, full - high], axis=0).astype(jnp.bfloat16)


def on_device(coords, charges, atom_types, counts, c6_table, c12_table):
    slots = coords.shape[-1]
    cells_x, cells_y, cells_z = coords.shape[:3]
    tables = make_tables(c6_table, c12_table, slots)
    occupied = jnp.arange(slots, dtype=jnp.int32) < counts[..., None]
    q = jnp.where(occupied, charges * ENERGY_UNIT**0.5, 0.0)
    kind = jnp.where(occupied, atom_types, slots - 1).astype(jnp.float32)
    held = jnp.broadcast_to(counts.astype(jnp.float32)[..., None], q.shape)
    rest = jnp.zeros(q.shape[:3] + (2, slots), jnp.float32)
    packed = jnp.concatenate(
        [coords, q[..., None, :], kind[..., None, :], held[..., None, :], rest], axis=3
    )
    extended = jnp.concatenate([packed, shifted(packed[:, :, :1], "gz", -1)], axis=2)
    side = shifted(extended[:, :1], "gy", -1)
    above = shifted(extended[:1], "gx", -1)
    corner = diagonal(extended[:1, :1])
    extended = jnp.concatenate(
        [jnp.concatenate([extended, side], axis=1), jnp.concatenate([above, corner], axis=1)], axis=0
    )
    row_counts = extended[:cells_x, :, :, 5, 0].astype(jnp.int32)
    forces = pair_call(row_counts, extended, tables)
    forces = give_back(forces, 2, "gz")
    forces = give_back(forces, 1, "gy")
    own = forces[0, 0, 0, 3]
    forces = give_back(forces, 0, "gx")
    return (forces[:, :, :, :3], jnp.sum(gathered(own, "gx", forces[0, 0, 0, 3])).reshape(1))


def diagonal(block):
    nx, ny = lax.axis_size("gx"), lax.axis_size("gy")
    route = [
        (((i + 1) % nx) * ny + (j + 1) % ny, i * ny + j) for i in range(nx) for j in range(ny)
    ]
    return lax.ppermute(block, ("gx", "gy"), route)


def gathered(own, axis, with_last):
    size = lax.axis_size(axis)
    if size == 1:
        return own
    if size > 4:
        return lax.psum(own, axis)
    for distance in range(2, size):
        with_last = with_last + shifted(own, axis, distance)
    return with_last


def give_back(forces, dim, axis):
    cells = forces.shape[dim] - 1
    kept = lax.slice_in_dim(forces, 0, cells, axis=dim)
    returned = shifted(lax.slice_in_dim(forces, cells, cells + 1, axis=dim), axis, 1)
    first = lax.slice_in_dim(kept, 0, 1, axis=dim) + returned
    if dim > 0 and lax.axis_size(axis) != 2:
        row = gathered(forces[0, 0, 0, 3], axis, first[0, 0, 0, 3])
        first = first.at[:, :, :, 3].set(row)
    return jnp.concatenate([first, lax.slice_in_dim(kept, 1, cells, axis=dim)], axis=dim)


def solution(mesh):
    return jax.shard_map(
        on_device,
        mesh=mesh,
        in_specs=(
            P(("groups", "gx"), "gy", "gz", None, None),
            P(("groups", "gx"), "gy", "gz", None),
            P(("groups", "gx"), "gy", "gz", None),
            P(("groups", "gx"), "gy", "gz"),
            P(),
            P(),
        ),
        out_specs=(P(("groups", "gx"), "gy", "gz", None, None), P("groups")),
        check_vma=False,
    )
```

```python
import jax
import jax.numpy as jnp
import numpy as np
from jax import lax
from jax.experimental import pallas as pl
from jax.experimental.pallas import tpu as pltpu
from jax.sharding import PartitionSpec as P

CELL_EDGE = 1.1
CUT_SQUARE = 1.0
SOFTEN = 0.09
ENERGY_UNIT = 0.1
EDGE_T = CUT_SQUARE + SOFTEN
K1 = EDGE_T**-0.5
K3 = EDGE_T**-3.0
K6 = EDGE_T**-6.0
OFFSETS = (
    (0, 0, 0),
    (0, 0, 1),
    (0, 1, 0),
    (0, 1, 1),
    (0, 1, -1),
) + tuple((1, oy, oz) for oy in (-1, 0, 1) for oz in (-1, 0, 1))
ROWS = 32
AXES = ("gx", "gy", "gz")


def moved(block, dx, dy, dz):
    nx, ny, nz = (lax.axis_size(a) for a in AXES)
    flat = lambda i, j, k: ((i % nx) * ny + j % ny) * nz + k % nz
    cells = [(i, j, k) for i in range(nx) for j in range(ny) for k in range(nz)]
    route = [(flat(i - dx, j - dy, k - dz), flat(i, j, k)) for i, j, k in cells]
    return lax.ppermute(block, AXES, route)


def pack_kernel(counts_ref, coords_ref, charges_ref, types_ref, packed_ref, faces_ref):
    cells_x, cells_y, _, cells_z, slots = coords_ref.shape
    lane = lax.broadcasted_iota(jnp.int32, (1, slots), 1)
    for ix in range(cells_x):
        for iy in range(cells_y):
            for iz in range(cells_z):
                here = lane < counts_ref[ix, iy, iz]
                q = jnp.where(here, charges_ref[ix, iy, iz : iz + 1] * ENERGY_UNIT**0.5, 0.0)
                kind = jnp.where(here, types_ref[ix, iy, iz : iz + 1], slots - 1).astype(jnp.float32)
                place = [coords_ref[ix, iy, k, iz : iz + 1] for k in range(3)]
                cell = jnp.concatenate(place + [q, kind, jnp.zeros((3, slots), jnp.float32)], axis=0)
                packed_ref[ix, iy, iz] = cell
                for b, at in enumerate((0, cells_z - 1)):
                    if iz == at:
                        faces_ref[ix, iy, b] = cell


def whole_call(kernel, name, outs, operands, smem=0):
    vmem = pl.BlockSpec(memory_space=pltpu.VMEM)
    return pl.pallas_call(
        kernel,
        out_shape=tuple(jax.ShapeDtypeStruct(o, jnp.float32) for o in outs),
        in_specs=[pl.BlockSpec(memory_space=pltpu.SMEM)] * smem + [vmem] * (len(operands) - smem),
        out_specs=(vmem,) * len(outs),
        name=name,
    )(*operands)


def row_kernel(packed_ref, c6_ref, c12_ref, left_ref, rows_ref, table_ref):
    cells_z, _, slots = packed_ref.shape[2:]
    f32, bf16 = jnp.float32, jnp.bfloat16
    row_id = lax.broadcasted_iota(jnp.int32, (8, slots), 0)
    lane_of = lax.broadcasted_iota(jnp.int32, (slots, slots), 1).astype(f32)
    ix, iy = pl.program_id(0), pl.program_id(1) + 1

    @pl.when((pl.program_id(0) == 0) & (pl.program_id(1) == 0))
    def _():
        kinds = c6_ref.shape[0]
        table_ref[...] = jnp.zeros_like(table_ref)
        c6, c12 = ((0.5 * ENERGY_UNIT) * (c[...] + c[...].T) for c in (c6_ref, c12_ref))
        for k, table in enumerate((c6 - c12 * K3, c12)):
            high = table.astype(bf16)
            at = slice(k * slots, k * slots + kinds)
            table_ref[0:kinds, at] = high
            table_ref[slots : slots + kinds, at] = (table - high.astype(f32)).astype(bf16)

    for iz in range(cells_z):
        at = jnp.where(row_id == 0, ix, jnp.where(row_id == 1, iy, jnp.where(row_id == 2, iz + 1, 0)))
        f = packed_ref[0, 0, iz] + at.astype(f32) * CELL_EDGE
        high = f.astype(bf16).astype(f32)
        mid = (f - high).astype(bf16).astype(f32)
        parts = jnp.concatenate([high, mid, f - high - mid], axis=0).T.astype(bf16)
        mine = jnp.dot(parts, left_ref[...], preferred_element_type=f32)
        hot = (mine[:, 4 * slots :] == lane_of).astype(f32).astype(bf16)
        looked = jnp.dot(jnp.concatenate([hot, hot], axis=1), table_ref[...], preferred_element_type=f32)
        for k in range(4):
            rows_ref[0, iz, k] = mine[:, k * slots : (k + 1) * slots]
        for k in range(2):
            rows_ref[0, iz, 4 + k] = looked[:, k * slots : (k + 1) * slots]


def row_call(packed, c6_table, c12_table):
    cells_x, cells_y, cells_z, _, slots = packed.shape
    left = np.zeros((24, 5 * slots), np.float32)
    for k in range(5):
        for n in range(3):
            left[8 * n + k, k * slots : (k + 1) * slots] = 1.0
    left = jnp.asarray(left, jnp.bfloat16)
    atoms = cells_x * cells_y * cells_z * slots
    return pl.pallas_call(
        row_kernel,
        grid=(cells_x, cells_y),
        out_shape=jax.ShapeDtypeStruct((cells_x * cells_y, cells_z, 6, slots, slots), jnp.float32),
        in_specs=[
            pl.BlockSpec((1, 1, cells_z, 8, slots), lambda i, j: (i, j, 0, 0, 0)),
            pl.BlockSpec(c6_table.shape, lambda i, j: (0, 0)),
            pl.BlockSpec(c12_table.shape, lambda i, j: (0, 0)),
            pl.BlockSpec(left.shape, lambda i, j: (0, 0)),
        ],
        out_specs=pl.BlockSpec((1, cells_z, 6, slots, slots), lambda i, j: (i * cells_y + j, 0, 0, 0, 0)),
        scratch_shapes=[pltpu.VMEM((2 * slots, 2 * slots), jnp.bfloat16)],
        cost_estimate=pl.CostEstimate(
            flops=2 * atoms * slots * 376, transcendentals=0, bytes_accessed=atoms * slots * 24
        ),
        name="row_operands",
    )(packed, c6_table, c12_table, left)


def pair_kernel(
    counts_ref, packed_ref, pz_ref, py_ref, px_ref, pc_ref, rows_ref,
    own_ref, oz_ref, oy_ref, ozy_ref, ox_ref, fa,
    fe, types, fb, eacc,
):
    cells_x, cells_y, cells_z, _, slots = own_ref.shape
    ext_y, ext_z = cells_y + 2, cells_z + 2
    f32, bf16 = jnp.float32, jnp.bfloat16
    row_id = lax.broadcasted_iota(jnp.int32, (8, slots), 0)
    line = pl.program_id(0)

    @pl.when(line == 0)
    def _():
        eacc[...] = jnp.zeros_like(eacc)

        def place(f, ix, iy, iz):
            at = jnp.where(row_id == 0, ix, jnp.where(row_id == 1, iy, jnp.where(row_id == 2, iz, 0)))
            fe[ix, iy, iz] = f + at.astype(f32) * CELL_EDGE
            types[ix, iy, iz] = f[4:5].astype(jnp.int32)
            fb[ix, iy, iz] = jnp.zeros(fb.shape[3:], f32)

        def place_line(iy, _):
            for ix in range(cells_x):
                for iz in range(cells_z):
                    place(packed_ref[ix, iy, iz], ix, iy + 1, iz + 1)
                place(pz_ref[ix, iy, 0], ix, iy + 1, cells_z + 1)
                place(pz_ref[ix, iy, 1], ix, iy + 1, 0)
            for iz in range(ext_z):
                place(px_ref[0, iy, iz], cells_x, iy + 1, iz)
            return 0

        lax.fori_loop(0, cells_y, place_line, 0)
        for iz in range(ext_z):
            for ix in range(cells_x):
                place(py_ref[ix, 0, iz], ix, cells_y + 1, iz)
                fb[ix, 0, iz] = jnp.zeros(fb.shape[3:], f32)
            place(pc_ref[0, 0, iz], cells_x, cells_y + 1, iz)
            place(pc_ref[0, 1, iz], cells_x, 0, iz)

    def row_cell(ix, iy, iz, slot, offsets):
        count = counts_ref[ix, iy, iz]
        quarters = (count + (ROWS // 4 - 1)) // (ROWS // 4)
        full = quarters // 4
        half = (quarters // 2) % 2
        rest = quarters % 2

        def chunk(at, energy, rows):
            at = pl.multiple_of(at, rows)
            here = pl.ds(at, rows)
            ax, ay, az, aq, a6, a12 = (rows_ref[0, slot, k, here, :] for k in range(6))
            fx = fy = fz = None
            for ox, oy, oz in offsets:
                cell = (ix + ox, iy + 1 + oy, iz + 1 + oz)
                spread = lambda k: jnp.broadcast_to(fe[cell[0], cell[1], cell[2], k : k + 1, :], (rows, slots))
                dx = spread(0) - ax
                dy = spread(1) - ay
                dz = spread(2) - az
                qq = spread(3) * aq
                kind = jnp.broadcast_to(types[cell[0], cell[1], cell[2]], (rows, slots))
                c6, c12 = (
                    jnp.take_along_axis(t, kind, axis=1, mode="promise_in_bounds") for t in (a6, a12)
                )
                t = dx * dx + dy * dy + (dz * dz + SOFTEN)
                y = lax.rsqrt(t)
                v = y * y
                v3 = v * v * v
                p = qq * y
                h = c12 * v3
                m = h - c6
                gap = v3 - K3
                u = qq * (y - K1) + gap * m
                z = p + (6.0 * v3) * (m + c12 * gap)
                w = jnp.maximum(EDGE_T - t, 0.0)
                if (ox, oy, oz) == (0, 0, 0):
                    lane = lax.broadcasted_iota(jnp.int32, (rows, slots), 1)
                    row = lax.broadcasted_iota(jnp.int32, (rows, slots), 0) + at
                    w = jnp.where(lane > row, w, 0.0)
                s = w * ((w * v) * z + 4.0 * u)
                e = w * (w * u)
                for r in range(0, rows, 8):
                    energy = energy + e[r : r + 8]
                px, py, pz = s * dx, s * dy, s * dz
                for k, part in enumerate((px, py, pz)):
                    fold = part[0:8]
                    for r in range(8, rows, 8):
                        fold = fold + part[r : r + 8]
                    fb[cell[0], cell[1], cell[2], k] = fb[cell[0], cell[1], cell[2], k] + fold
                if fx is None:
                    fx, fy, fz = px, py, pz
                else:
                    fx, fy, fz = fx + px, fy + py, fz + pz
            for k, part in enumerate((fx, fy, fz)):
                fa[0, slot, k, here, :] = part
            return energy

        energy = lax.fori_loop(0, full, lambda c, e: chunk(c * ROWS, e, ROWS), eacc[...])
        energy = lax.fori_loop(0, half, lambda c, e: chunk(full * ROWS, e, ROWS // 2), energy)
        last = full * ROWS + half * (ROWS // 2)
        eacc[...] = lax.fori_loop(0, rest, lambda c, e: chunk(last, e, ROWS // 4), energy)

    ix = line // cells_y
    iy = line % cells_y
    fa[...] = jnp.zeros_like(fa)

    def inner(iz, _):
        row_cell(ix, iy, iz, iz, OFFSETS)
        return 0

    lax.fori_loop(0, cells_z, inner, 0)
    @pl.when(line == pl.num_programs(0) - 1)
    def _():
        energy = jnp.sum(eacc[...], axis=0, keepdims=True)

        def total_of(ix, iy, iz):
            parts = [jnp.sum(fb[ix, iy, iz, k], axis=0, keepdims=True) for k in range(3)]
            return jnp.concatenate(parts + [energy, jnp.zeros((4, slots), f32)], axis=0)

        def close_line(iy, _):
            for ix in range(cells_x + 1):
                for iz in range(cells_z):
                    if ix < cells_x:
                        own_ref[ix, iy, iz] = total_of(ix, iy + 1, iz + 1)
                    else:
                        ox_ref[0, iy, iz] = total_of(ix, iy + 1, iz + 1)
                for b, at_z in enumerate((0, cells_z + 1)):
                    oz_ref[ix, iy, b] = total_of(ix, iy + 1, at_z)
            return 0

        lax.fori_loop(0, cells_y, close_line, 0)
        for ix in range(cells_x + 1):
            for a, at_y in enumerate((0, cells_y + 1)):
                for iz in range(cells_z):
                    oy_ref[ix, a, iz] = total_of(ix, at_y, iz + 1)
                for b, at_z in enumerate((0, cells_z + 1)):
                    ozy_ref[ix, a, b] = total_of(ix, at_y, at_z)


def pair_call(counts, pieces, rows):
    cells_x, cells_y, cells_z = counts.shape
    slots = rows.shape[-1]
    f32 = jnp.float32
    fixed = lambda shape: pl.BlockSpec(shape, lambda i: (0,) * len(shape))
    outs = [
        dims + (8, slots)
        for dims in (
            (cells_x, cells_y, cells_z),
            (cells_x + 1, cells_y, 2),
            (cells_x + 1, 2, cells_z),
            (cells_x + 1, 2, 2),
            (1, cells_y, cells_z),
        )
    ]
    sums = (cells_x * cells_y, cells_z, 3, slots, slots)
    by_line = lambda shape: pl.BlockSpec((1,) + shape[1:], lambda i: (i, 0, 0, 0, 0))
    grown = (cells_x + 1, cells_y + 2, cells_z + 2)
    return pl.pallas_call(
        pair_kernel,
        grid=(cells_x * cells_y,),
        out_shape=tuple(jax.ShapeDtypeStruct(o, f32) for o in outs + [sums]),
        in_specs=[pl.BlockSpec(memory_space=pltpu.SMEM)]
        + [fixed(piece.shape) for piece in pieces]
        + [by_line(rows.shape)],
        out_specs=tuple(fixed(o) for o in outs) + (by_line(sums),),
        scratch_shapes=[
            pltpu.VMEM(grown + (8, slots), f32),
            pltpu.VMEM(grown + (1, slots), jnp.int32),
            pltpu.VMEM(grown + (3, 8, slots), f32),
            pltpu.VMEM((8, slots), f32),
        ],
        name="pair_forces",
    )(counts, *pieces, rows)


def own_kernel(sums_ref, own_ref, ends_ref, out_ref):
    f32, bf16 = jnp.float32, jnp.bfloat16
    for iz in range(sums_ref.shape[1]):
        halves = []
        for k in range(3):
            whole = sums_ref[0, iz, k]
            high = whole.astype(bf16)
            halves += [high, (whole - high.astype(f32)).astype(bf16)]
        total = jnp.dot(jnp.concatenate(halves, axis=1), ends_ref[...], preferred_element_type=f32)
        out_ref[0, 0, iz] = own_ref[0, 0, iz] - total.T[:8]


def own_call(sums, own):
    cells_x, cells_y, cells_z, _, slots = own.shape
    ends = np.zeros((6 * slots, slots), np.float32)
    for k in range(3):
        ends[2 * k * slots : 2 * (k + 1) * slots, k] = 1.0
    ends = jnp.asarray(ends, jnp.bfloat16)
    block = pl.BlockSpec((1, 1, cells_z, 8, slots), lambda i, j: (i, j, 0, 0, 0))
    return pl.pallas_call(
        own_kernel,
        grid=(cells_x, cells_y),
        out_shape=jax.ShapeDtypeStruct(own.shape, jnp.float32),
        in_specs=[
            pl.BlockSpec((1,) + sums.shape[1:], lambda i, j: (i * cells_y + j, 0, 0, 0, 0)),
            block,
            pl.BlockSpec(ends.shape, lambda i, j: (0, 0)),
        ],
        out_specs=block,
        cost_estimate=pl.CostEstimate(
            flops=8 * sums.size, transcendentals=0, bytes_accessed=4 * sums.size
        ),
        name="own_rows",
    )(sums, own, ends)


def final_kernel(own_ref, rz_ref, ry_ref, rzy_ref, rx_ref, *refs):
    *terms, forces_ref, energy_ref = refs
    cells_x, cells_y, cells_z, _, slots = own_ref.shape
    for ix in range(cells_x):
        for iy in range(cells_y):
            sides_y = [m for m, at in enumerate((cells_y - 1, 0)) if iy == at]
            for iz in range(cells_z):
                sides_z = [n for n, at in enumerate((cells_z - 1, 0)) if iz == at]
                f = own_ref[ix, iy, iz]
                for n in sides_z:
                    f = f + rz_ref[ix, iy, n]
                for m in sides_y:
                    f = f + ry_ref[ix, m, iz]
                    for n in sides_z:
                        f = f + rzy_ref[ix, m, n]
                if ix == 0:
                    f = f + rx_ref[0, iy, iz]
                if ix == 0 and iy == 0 and iz == 0:
                    energy = f[3:4]
                for k in range(3):
                    forces_ref[ix, iy, k, iz : iz + 1] = f[k : k + 1]
    for term in terms:
        energy = energy + term[...]
    energy_ref[...] = jnp.broadcast_to(jnp.sum(energy, axis=1, keepdims=True), (1, slots))


def both_ways(block, dim, step, size):
    if size == 2:
        return moved(block, *step)
    down = moved(lax.slice_in_dim(block, 0, 1, axis=dim), *(-d for d in step))
    up = moved(lax.slice_in_dim(block, 1, 2, axis=dim), *step)
    return jnp.concatenate([down, up], axis=dim)


def to_sides(z, y, zy, ny, nz):
    if ny == 2 and nz == 2:
        corners = moved(zy, 0, 1, 1)
    else:
        corners = jnp.concatenate(
            [
                jnp.concatenate(
                    [moved(zy[:, a : a + 1, b : b + 1], 0, 2 * a - 1, 2 * b - 1) for b in range(2)], axis=2
                )
                for a in range(2)
            ],
            axis=1,
        )
    return both_ways(z, 2, (0, 0, 1), nz), both_ways(y, 1, (0, 1, 0), ny), corners


def spread(block, dim, size):
    zeros = jnp.zeros(block.shape[:dim] + (size - 2,) + block.shape[dim + 1 :], block.dtype)
    down, up = (lax.slice_in_dim(block, m, m + 1, axis=dim) for m in range(2))
    return jnp.concatenate([up, zeros, down], axis=dim)


def on_device(coords, charges, atom_types, counts, c6_table, c12_table):
    slots = coords.shape[-1]
    cells_x, cells_y, cells_z = coords.shape[:3]
    nx, ny, nz = (lax.axis_size(a) for a in AXES)
    tail = (8, slots)
    packed, faces = whole_call(
        pack_kernel,
        "pack_cells",
        [(cells_x, cells_y, cells_z) + tail, (cells_x, cells_y, 2) + tail],
        (counts, jnp.swapaxes(coords, 2, 3), charges, atom_types),
        smem=1,
    )
    pz = both_ways(faces, 2, (0, 0, 1), nz)
    lines = jnp.concatenate([pz[:, :, 1:], packed, pz[:, :, :1]], axis=2)
    ends = jnp.concatenate([lines[:1, :1], lines[:1, cells_y - 1 :]], axis=1)
    px = moved(lines[:1], -1, 0, 0)
    py = moved(lines[:, :1], 0, -1, 0)
    if ny == 2:
        pc = moved(ends, -1, -1, 0)
    else:
        pc = jnp.concatenate([moved(ends[:, :1], -1, -1, 0), moved(ends[:, 1:], -1, 1, 0)], axis=1)
    rows = row_call(packed, c6_table, c12_table)
    own, oz, oy, ozy, ox, sums = pair_call(counts, (packed, pz, py, px, pc), rows)
    rz, ry, rzy = to_sides(oz, oy, ozy, ny, nz)
    own, rz = lax.optimization_barrier((own_call(sums, own), rz))
    ox = (
        ox
        + spread(rz[cells_x:], 2, cells_z)
        + spread(ry[cells_x:], 1, cells_y)
        + spread(spread(rzy[cells_x:], 2, cells_z), 1, cells_y)
    )
    rx = moved(ox, 1, 0, 0)
    if nz == 2 and ny == 2 and 2 <= nx <= 4:
        summed = ox[0, 0, 0, 3:4]
        terms = [moved(summed, i, 0, 0) for i in range(2, nx)]
    else:
        terms = [lax.psum(own[0, 0, 0, 3:4], AXES)]
        rz, ry, rzy, rx = (r.at[..., 3, :].set(0.0) for r in (rz, ry, rzy, rx))
        own = own.at[..., 3, :].set(0.0)
    forces, energy = whole_call(
        final_kernel,
        "join_forces",
        [(cells_x, cells_y, 3, cells_z, slots), (1, slots)],
        (own, rz, ry, rzy, rx, *terms),
    )
    return (jnp.swapaxes(forces, 2, 3), energy[0, :1])


def solution(mesh):
    return jax.shard_map(
        on_device,
        mesh=mesh,
        in_specs=(
            P(("groups", "gx"), "gy", "gz", None, None),
            P(("groups", "gx"), "gy", "gz", None),
            P(("groups", "gx"), "gy", "gz", None),
            P(("groups", "gx"), "gy", "gz"),
            P(),
            P(),
        ),
        out_specs=(P(("groups", "gx"), "gy", "gz", None, None), P("groups")),
        check_vma=False,
    )
```

```python
import jax
import jax.numpy as jnp
import numpy as np
from jax import lax
from jax.experimental import pallas as pl
from jax.experimental.pallas import tpu as pltpu
from jax.sharding import PartitionSpec as P

CELL_EDGE = 1.1
CUT_SQUARE = 1.0
SOFTEN = 0.09
ENERGY_UNIT = 0.1
EDGE_T = CUT_SQUARE + SOFTEN
K1 = EDGE_T**-0.5
K3 = EDGE_T**-3.0
K6 = EDGE_T**-6.0
OFFSETS = (
    (0, 0, 1),
    (0, 1, 0),
    (0, 1, 1),
    (0, 1, -1),
) + tuple((1, oy, oz) for oy in (-1, 0, 1) for oz in (-1, 0, 1))
ROWS = 32
AXES = ("gx", "gy", "gz")


def moved(block, dx, dy, dz):
    nx, ny, nz = (lax.axis_size(a) for a in AXES)
    flat = lambda i, j, k: ((i % nx) * ny + j % ny) * nz + k % nz
    cells = [(i, j, k) for i in range(nx) for j in range(ny) for k in range(nz)]
    route = [(flat(i - dx, j - dy, k - dz), flat(i, j, k)) for i, j, k in cells]
    return lax.ppermute(block, AXES, route)


def pack_kernel(counts_ref, coords_ref, charges_ref, types_ref, packed_ref, faces_ref):
    cells_x, cells_y, _, cells_z, slots = coords_ref.shape
    lane = lax.broadcasted_iota(jnp.int32, (1, slots), 1)
    for ix in range(cells_x):
        for iy in range(cells_y):
            for iz in range(cells_z):
                here = lane < counts_ref[ix, iy, iz]
                q = jnp.where(here, charges_ref[ix, iy, iz : iz + 1] * ENERGY_UNIT**0.5, 0.0)
                kind = jnp.where(here, types_ref[ix, iy, iz : iz + 1], slots - 1).astype(jnp.float32)
                place = [coords_ref[ix, iy, k, iz : iz + 1] for k in range(3)]
                cell = jnp.concatenate(place + [q, kind, jnp.zeros((3, slots), jnp.float32)], axis=0)
                packed_ref[ix, iy, iz] = cell
                for b, at in enumerate((0, cells_z - 1)):
                    if iz == at:
                        faces_ref[ix, iy, b] = cell


def whole_call(kernel, name, outs, operands, smem=0):
    vmem = pl.BlockSpec(memory_space=pltpu.VMEM)
    return pl.pallas_call(
        kernel,
        out_shape=tuple(jax.ShapeDtypeStruct(o, jnp.float32) for o in outs),
        in_specs=[pl.BlockSpec(memory_space=pltpu.SMEM)] * smem + [vmem] * (len(operands) - smem),
        out_specs=(vmem,) * len(outs),
        name=name,
    )(*operands)


def pair_terms(dx, dy, dz, qq, c6, c12, kept=None):
    t = dx * dx + dy * dy + (dz * dz + SOFTEN)
    y = lax.rsqrt(t)
    v = y * y
    v3 = v * v * v
    p = qq * y
    h = c12 * v3
    m = h - c6
    gap = v3 - K3
    u = qq * (y - K1) + gap * m
    z = p + (6.0 * v3) * (m + c12 * gap)
    w = jnp.maximum(EDGE_T - t, 0.0)
    if kept is not None:
        w = jnp.where(kept, w, 0.0)
    return w * ((w * v) * z + 4.0 * u), w * (w * u)


def row_kernel(packed_ref, c6_ref, c12_ref, left_ref, rows_hbm, self_ref, energy_ref, table_ref, rows_ref, sem):
    cells_x, cells_y, cells_z, _, slots = packed_ref.shape
    f32, bf16 = jnp.float32, jnp.bfloat16
    row_id = lax.broadcasted_iota(jnp.int32, (8, slots), 0)
    lane = lax.broadcasted_iota(jnp.int32, (8, slots), 1)
    lane_of = lax.broadcasted_iota(jnp.int32, (cells_z * slots, slots), 1).astype(f32)
    lines = cells_x * cells_y

    kinds = c6_ref.shape[0]
    table_ref[...] = jnp.zeros_like(table_ref)
    c6, c12 = ((0.5 * ENERGY_UNIT) * (c[...] + c[...].T) for c in (c6_ref, c12_ref))
    for k, table in enumerate((c6 - c12 * K3, c12)):
        high = table.astype(bf16)
        at = slice(k * slots, k * slots + kinds)
        table_ref[0:kinds, at] = high
        table_ref[slots : slots + kinds, at] = (table - high.astype(f32)).astype(bf16)

    def store(line):
        slot = line % 2
        return pltpu.make_async_copy(rows_ref.at[slot], rows_hbm.at[line], sem.at[slot])

    def do_line(line, energy):
        ix, iy, slot = line // cells_y, line % cells_y, line % 2

        def placed(iz):
            at = jnp.where(row_id == 0, ix, jnp.where(row_id == 1, iy + 1, jnp.where(row_id == 2, iz + 1, 0)))
            return packed_ref[ix, iy, iz] + at.astype(f32) * CELL_EDGE

        @pl.when(line >= 2)
        def _():
            store(line - 2).wait()

        def split(iz):
            f = placed(iz)
            high = f.astype(bf16).astype(f32)
            mid = (f - high).astype(bf16).astype(f32)
            return jnp.concatenate([high, mid, f - high - mid], axis=0).T.astype(bf16)

        parts = jnp.concatenate([split(iz) for iz in range(cells_z)], axis=0)
        cut = lambda product, k: product[:, k * slots : (k + 1) * slots].reshape(cells_z, slots, slots)
        kinds_of = jnp.dot(parts, left_ref[:, 4 * slots :], preferred_element_type=f32)
        hot = (kinds_of == lane_of).astype(f32).astype(bf16)
        for first in (0, 2):
            mine = jnp.dot(
                parts, left_ref[:, first * slots : (first + 2) * slots], preferred_element_type=f32
            )
            for k in range(2):
                rows_ref[slot, :, first + k] = cut(mine, k)
        looked = jnp.dot(jnp.concatenate([hot, hot], axis=1), table_ref[...], preferred_element_type=f32)
        for k in range(2):
            rows_ref[slot, :, 4 + k] = cut(looked, k)
        store(line).start()

        def inside(iz, energy):
            f = placed(iz)
            bx, by, bz, bq = (jnp.broadcast_to(f[k : k + 1], (8, slots)) for k in range(4))
            kind = jnp.broadcast_to(f[4:5].astype(jnp.int32), (8, slots))
            fold = None
            for at in range(0, slots, 8):
                ax, ay, az, aq, a6, a12 = (rows_ref[slot, iz, k, at : at + 8, :] for k in range(6))
                dx, dy, dz = bx - ax, by - ay, bz - az
                c6, c12 = (
                    jnp.take_along_axis(t, kind, axis=1, mode="promise_in_bounds") for t in (a6, a12)
                )
                s, e = pair_terms(dx, dy, dz, bq * aq, c6, c12, lane != row_id + at)
                energy = energy + e
                moved = (s * dx, s * dy, s * dz)
                fold = moved if fold is None else tuple(a + b for a, b in zip(fold, moved))
            for k in range(3):
                self_ref[line, iz, k] = fold[k]
            return energy

        return lax.fori_loop(0, cells_z, inside, energy)

    energy = lax.fori_loop(0, lines, do_line, jnp.zeros((8, slots), f32))
    energy_ref[...] = 0.5 * energy
    for line in range(max(lines - 2, 0), lines):
        store(line).wait()


def row_call(packed, c6_table, c12_table):
    cells_x, cells_y, cells_z, _, slots = packed.shape
    left = np.zeros((24, 5 * slots), np.float32)
    for k in range(5):
        for n in range(3):
            left[8 * n + k, k * slots : (k + 1) * slots] = 1.0
    left = jnp.asarray(left, jnp.bfloat16)
    atoms = cells_x * cells_y * cells_z * slots
    line = (cells_z, 6, slots, slots)
    vmem = pl.BlockSpec(memory_space=pltpu.VMEM)
    return pl.pallas_call(
        row_kernel,
        out_shape=(
            jax.ShapeDtypeStruct((cells_x * cells_y,) + line, jnp.float32),
            jax.ShapeDtypeStruct((cells_x * cells_y, cells_z, 3, 8, slots), jnp.float32),
            jax.ShapeDtypeStruct((8, slots), jnp.float32),
        ),
        in_specs=[vmem] * 4,
        out_specs=(pl.BlockSpec(memory_space=pl.ANY), vmem, vmem),
        scratch_shapes=[
            pltpu.VMEM((2 * slots, 2 * slots), jnp.bfloat16),
            pltpu.VMEM((2,) + line, jnp.float32),
            pltpu.SemaphoreType.DMA((2,)),
        ],
        cost_estimate=pl.CostEstimate(
            flops=2 * atoms * slots * 376, transcendentals=0, bytes_accessed=atoms * slots * 24
        ),
        name="row_operands",
    )(packed, c6_table, c12_table, left)


def pair_kernel(
    counts_ref, packed_ref, pz_ref, py_ref, px_ref, pc_ref, self_ref, energy_ref, rows_ref,
    own_ref, oz_ref, oy_ref, ozy_ref, ox_ref, fa,
    fe, types, fb, eacc,
):
    cells_x, cells_y, cells_z, _, slots = own_ref.shape
    ext_y, ext_z = cells_y + 2, cells_z + 2
    f32, bf16 = jnp.float32, jnp.bfloat16
    row_id = lax.broadcasted_iota(jnp.int32, (8, slots), 0)
    line = pl.program_id(0)

    @pl.when(line == 0)
    def _():
        eacc[...] = energy_ref[...]

        def place(f, ix, iy, iz):
            at = jnp.where(row_id == 0, ix, jnp.where(row_id == 1, iy, jnp.where(row_id == 2, iz, 0)))
            fe[ix, iy, iz] = f + at.astype(f32) * CELL_EDGE
            types[ix, iy, iz] = f[4:5].astype(jnp.int32)
            fb[ix, iy, iz] = jnp.zeros(fb.shape[3:], f32)

        def place_line(iy, _):
            for ix in range(cells_x):
                for iz in range(cells_z):
                    place(packed_ref[ix, iy, iz], ix, iy + 1, iz + 1)
                    fb[ix, iy + 1, iz + 1] = self_ref[ix * cells_y + iy, iz]
                place(pz_ref[ix, iy, 0], ix, iy + 1, cells_z + 1)
                place(pz_ref[ix, iy, 1], ix, iy + 1, 0)
            for iz in range(ext_z):
                place(px_ref[0, iy, iz], cells_x, iy + 1, iz)
            return 0

        lax.fori_loop(0, cells_y, place_line, 0)
        for iz in range(ext_z):
            for ix in range(cells_x):
                place(py_ref[ix, 0, iz], ix, cells_y + 1, iz)
                fb[ix, 0, iz] = jnp.zeros(fb.shape[3:], f32)
            place(pc_ref[0, 0, iz], cells_x, cells_y + 1, iz)
            place(pc_ref[0, 1, iz], cells_x, 0, iz)

    def row_cell(ix, iy, iz, slot, offsets):
        count = counts_ref[ix, iy, iz]
        quarters = (count + (ROWS // 4 - 1)) // (ROWS // 4)
        full = quarters // 4
        half = (quarters // 2) % 2
        rest = quarters % 2

        def chunk(at, energy, rows):
            at = pl.multiple_of(at, rows)
            here = pl.ds(at, rows)
            ax, ay, az, aq, a6, a12 = (rows_ref[0, slot, k, here, :] for k in range(6))
            fx = fy = fz = None
            for ox, oy, oz in offsets:
                cell = (ix + ox, iy + 1 + oy, iz + 1 + oz)
                spread = lambda k: jnp.broadcast_to(fe[cell[0], cell[1], cell[2], k : k + 1, :], (rows, slots))
                dx = spread(0) - ax
                dy = spread(1) - ay
                dz = spread(2) - az
                qq = spread(3) * aq
                kind = jnp.broadcast_to(types[cell[0], cell[1], cell[2]], (rows, slots))
                c6, c12 = (
                    jnp.take_along_axis(t, kind, axis=1, mode="promise_in_bounds") for t in (a6, a12)
                )
                s, e = pair_terms(dx, dy, dz, qq, c6, c12)
                for r in range(0, rows, 8):
                    energy = energy + e[r : r + 8]
                px, py, pz = s * dx, s * dy, s * dz
                for k, part in enumerate((px, py, pz)):
                    fold = part[0:8]
                    for r in range(8, rows, 8):
                        fold = fold + part[r : r + 8]
                    fb[cell[0], cell[1], cell[2], k] = fb[cell[0], cell[1], cell[2], k] + fold
                if fx is None:
                    fx, fy, fz = px, py, pz
                else:
                    fx, fy, fz = fx + px, fy + py, fz + pz
            for k, part in enumerate((fx, fy, fz)):
                fa[0, slot, k, here, :] = part
            return energy

        energy = lax.fori_loop(0, full, lambda c, e: chunk(c * ROWS, e, ROWS), eacc[...])
        energy = lax.fori_loop(0, half, lambda c, e: chunk(full * ROWS, e, ROWS // 2), energy)
        last = full * ROWS + half * (ROWS // 2)
        eacc[...] = lax.fori_loop(0, rest, lambda c, e: chunk(last, e, ROWS // 4), energy)

    ix = line // cells_y
    iy = line % cells_y
    fa[...] = jnp.zeros_like(fa)

    def inner(iz, _):
        row_cell(ix, iy, iz, iz, OFFSETS)
        return 0

    lax.fori_loop(0, cells_z, inner, 0)
    @pl.when(line == pl.num_programs(0) - 1)
    def _():
        energy = jnp.sum(eacc[...], axis=0, keepdims=True)

        def total_of(ix, iy, iz):
            parts = [jnp.sum(fb[ix, iy, iz, k], axis=0, keepdims=True) for k in range(3)]
            return jnp.concatenate(parts + [energy, jnp.zeros((4, slots), f32)], axis=0)

        def close_line(iy, _):
            for ix in range(cells_x + 1):
                for iz in range(cells_z):
                    if ix < cells_x:
                        own_ref[ix, iy, iz] = total_of(ix, iy + 1, iz + 1)
                    else:
                        ox_ref[0, iy, iz] = total_of(ix, iy + 1, iz + 1)
                for b, at_z in enumerate((0, cells_z + 1)):
                    oz_ref[ix, iy, b] = total_of(ix, iy + 1, at_z)
            return 0

        lax.fori_loop(0, cells_y, close_line, 0)
        for ix in range(cells_x + 1):
            for a, at_y in enumerate((0, cells_y + 1)):
                for iz in range(cells_z):
                    oy_ref[ix, a, iz] = total_of(ix, at_y, iz + 1)
                for b, at_z in enumerate((0, cells_z + 1)):
                    ozy_ref[ix, a, b] = total_of(ix, at_y, at_z)


def pair_call(counts, pieces, rows, inside, energy):
    cells_x, cells_y, cells_z = counts.shape
    slots = rows.shape[-1]
    f32 = jnp.float32
    fixed = lambda shape: pl.BlockSpec(shape, lambda i: (0,) * len(shape))
    outs = [
        dims + (8, slots)
        for dims in (
            (cells_x, cells_y, cells_z),
            (cells_x + 1, cells_y, 2),
            (cells_x + 1, 2, cells_z),
            (cells_x + 1, 2, 2),
            (1, cells_y, cells_z),
        )
    ]
    sums = (cells_x * cells_y, cells_z, 3, slots, slots)
    by_line = lambda shape: pl.BlockSpec((1,) + shape[1:], lambda i: (i, 0, 0, 0, 0))
    grown = (cells_x + 1, cells_y + 2, cells_z + 2)
    return pl.pallas_call(
        pair_kernel,
        grid=(cells_x * cells_y,),
        out_shape=tuple(jax.ShapeDtypeStruct(o, f32) for o in outs + [sums]),
        in_specs=[pl.BlockSpec(memory_space=pltpu.SMEM)]
        + [fixed(piece.shape) for piece in (*pieces, inside, energy)]
        + [by_line(rows.shape)],
        out_specs=tuple(fixed(o) for o in outs) + (by_line(sums),),
        scratch_shapes=[
            pltpu.VMEM(grown + (8, slots), f32),
            pltpu.VMEM(grown + (1, slots), jnp.int32),
            pltpu.VMEM(grown + (3, 8, slots), f32),
            pltpu.VMEM((8, slots), f32),
        ],
        name="pair_forces",
    )(counts, *pieces, inside, energy, rows)


def own_kernel(sums_ref, own_ref, ends_ref, out_ref):
    f32, bf16 = jnp.float32, jnp.bfloat16
    for iz in range(sums_ref.shape[1]):
        halves = []
        for k in range(3):
            whole = sums_ref[0, iz, k]
            high = whole.astype(bf16)
            halves += [high, (whole - high.astype(f32)).astype(bf16)]
        total = jnp.dot(jnp.concatenate(halves, axis=1), ends_ref[...], preferred_element_type=f32)
        out_ref[0, 0, iz] = own_ref[0, 0, iz] - total.T[:8]


def own_call(sums, own):
    cells_x, cells_y, cells_z, _, slots = own.shape
    ends = np.zeros((6 * slots, slots), np.float32)
    for k in range(3):
        ends[2 * k * slots : 2 * (k + 1) * slots, k] = 1.0
    ends = jnp.asarray(ends, jnp.bfloat16)
    block = pl.BlockSpec((1, 1, cells_z, 8, slots), lambda i, j: (i, j, 0, 0, 0))
    return pl.pallas_call(
        own_kernel,
        grid=(cells_x, cells_y),
        out_shape=jax.ShapeDtypeStruct(own.shape, jnp.float32),
        in_specs=[
            pl.BlockSpec((1,) + sums.shape[1:], lambda i, j: (i * cells_y + j, 0, 0, 0, 0)),
            block,
            pl.BlockSpec(ends.shape, lambda i, j: (0, 0)),
        ],
        out_specs=block,
        cost_estimate=pl.CostEstimate(
            flops=8 * sums.size, transcendentals=0, bytes_accessed=4 * sums.size
        ),
        name="own_rows",
    )(sums, own, ends)


def final_kernel(own_ref, rz_ref, ry_ref, rzy_ref, rx_ref, *refs):
    *terms, forces_ref, energy_ref = refs
    cells_x, cells_y, cells_z, _, slots = own_ref.shape
    for ix in range(cells_x):
        for iy in range(cells_y):
            sides_y = [m for m, at in enumerate((cells_y - 1, 0)) if iy == at]
            for iz in range(cells_z):
                sides_z = [n for n, at in enumerate((cells_z - 1, 0)) if iz == at]
                f = own_ref[ix, iy, iz]
                for n in sides_z:
                    f = f + rz_ref[ix, iy, n]
                for m in sides_y:
                    f = f + ry_ref[ix, m, iz]
                    for n in sides_z:
                        f = f + rzy_ref[ix, m, n]
                if ix == 0:
                    f = f + rx_ref[0, iy, iz]
                if ix == 0 and iy == 0 and iz == 0:
                    energy = f[3:4]
                for k in range(3):
                    forces_ref[ix, iy, k, iz : iz + 1] = f[k : k + 1]
    for term in terms:
        energy = energy + term[...]
    energy_ref[...] = jnp.broadcast_to(jnp.sum(energy, axis=1, keepdims=True), (1, slots))


def both_ways(block, dim, step, size):
    if size == 2:
        return moved(block, *step)
    down = moved(lax.slice_in_dim(block, 0, 1, axis=dim), *(-d for d in step))
    up = moved(lax.slice_in_dim(block, 1, 2, axis=dim), *step)
    return jnp.concatenate([down, up], axis=dim)


def to_sides(z, y, zy, ny, nz):
    if ny == 2 and nz == 2:
        corners = moved(zy, 0, 1, 1)
    else:
        corners = jnp.concatenate(
            [
                jnp.concatenate(
                    [moved(zy[:, a : a + 1, b : b + 1], 0, 2 * a - 1, 2 * b - 1) for b in range(2)], axis=2
                )
                for a in range(2)
            ],
            axis=1,
        )
    return both_ways(z, 2, (0, 0, 1), nz), both_ways(y, 1, (0, 1, 0), ny), corners


def spread(block, dim, size):
    zeros = jnp.zeros(block.shape[:dim] + (size - 2,) + block.shape[dim + 1 :], block.dtype)
    down, up = (lax.slice_in_dim(block, m, m + 1, axis=dim) for m in range(2))
    return jnp.concatenate([up, zeros, down], axis=dim)


def on_device(coords, charges, atom_types, counts, c6_table, c12_table):
    slots = coords.shape[-1]
    cells_x, cells_y, cells_z = coords.shape[:3]
    nx, ny, nz = (lax.axis_size(a) for a in AXES)
    tail = (8, slots)
    packed, faces = whole_call(
        pack_kernel,
        "pack_cells",
        [(cells_x, cells_y, cells_z) + tail, (cells_x, cells_y, 2) + tail],
        (counts, jnp.swapaxes(coords, 2, 3), charges, atom_types),
        smem=1,
    )
    pz = both_ways(faces, 2, (0, 0, 1), nz)
    lines = jnp.concatenate([pz[:, :, 1:], packed, pz[:, :, :1]], axis=2)
    ends = jnp.concatenate([lines[:1, :1], lines[:1, cells_y - 1 :]], axis=1)
    px = moved(lines[:1], -1, 0, 0)
    py = moved(lines[:, :1], 0, -1, 0)
    if ny == 2:
        pc = moved(ends, -1, -1, 0)
    else:
        pc = jnp.concatenate([moved(ends[:, :1], -1, -1, 0), moved(ends[:, 1:], -1, 1, 0)], axis=1)
    rows, inside, within = row_call(packed, c6_table, c12_table)
    own, oz, oy, ozy, ox, sums = pair_call(
        counts, (packed, pz, py, px, pc), rows, inside, within
    )
    rz, ry, rzy = to_sides(oz, oy, ozy, ny, nz)
    own, rz = lax.optimization_barrier((own_call(sums, own), rz))
    ox = (
        ox
        + spread(rz[cells_x:], 2, cells_z)
        + spread(ry[cells_x:], 1, cells_y)
        + spread(spread(rzy[cells_x:], 2, cells_z), 1, cells_y)
    )
    rx = moved(ox, 1, 0, 0)
    if nz == 2 and ny == 2 and 2 <= nx <= 4:
        summed = ox[0, 0, 0, 3:4]
        terms = [moved(summed, i, 0, 0) for i in range(2, nx)]
    else:
        terms = [lax.psum(own[0, 0, 0, 3:4], AXES)]
        rz, ry, rzy, rx = (r.at[..., 3, :].set(0.0) for r in (rz, ry, rzy, rx))
        own = own.at[..., 3, :].set(0.0)
    forces, energy = whole_call(
        final_kernel,
        "join_forces",
        [(cells_x, cells_y, 3, cells_z, slots), (1, slots)],
        (own, rz, ry, rzy, rx, *terms),
    )
    return (jnp.swapaxes(forces, 2, 3), energy[0, :1])


def solution(mesh):
    return jax.shard_map(
        on_device,
        mesh=mesh,
        in_specs=(
            P(("groups", "gx"), "gy", "gz", None, None),
            P(("groups", "gx"), "gy", "gz", None),
            P(("groups", "gx"), "gy", "gz", None),
            P(("groups", "gx"), "gy", "gz"),
            P(),
            P(),
        ),
        out_specs=(P(("groups", "gx"), "gy", "gz", None, None), P("groups")),
        check_vma=False,
    )
```

```python
import jax
import jax.numpy as jnp
import numpy as np
from jax import lax
from jax.experimental import pallas as pl
from jax.experimental.pallas import tpu as pltpu
from jax.sharding import PartitionSpec as P

CELL_EDGE = 1.1
CUT_SQUARE = 1.0
SOFTEN = 0.09
ENERGY_UNIT = 0.1
EDGE_T = CUT_SQUARE + SOFTEN
K1 = EDGE_T**-0.5
K3 = EDGE_T**-3.0
K6 = EDGE_T**-6.0
OFFSETS = (
    (0, 0, 1),
    (0, 1, 0),
    (0, 1, 1),
    (0, 1, -1),
) + tuple((1, oy, oz) for oy in (-1, 0, 1) for oz in (-1, 0, 1))
ROWS = 32
AXES = ("gx", "gy", "gz")


def moved(block, dx, dy, dz):
    nx, ny, nz = (lax.axis_size(a) for a in AXES)
    flat = lambda i, j, k: ((i % nx) * ny + j % ny) * nz + k % nz
    cells = [(i, j, k) for i in range(nx) for j in range(ny) for k in range(nz)]
    route = [(flat(i - dx, j - dy, k - dz), flat(i, j, k)) for i, j, k in cells]
    return lax.ppermute(block, AXES, route)


def pack_kernel(counts_ref, coords_ref, charges_ref, types_ref, packed_ref, faces_ref):
    cells_x, cells_y, _, cells_z, slots = coords_ref.shape
    lane = lax.broadcasted_iota(jnp.int32, (1, slots), 1)
    for ix in range(cells_x):
        for iy in range(cells_y):
            for iz in range(cells_z):
                here = lane < counts_ref[ix, iy, iz]
                q = jnp.where(here, charges_ref[ix, iy, iz : iz + 1] * ENERGY_UNIT**0.5, 0.0)
                kind = jnp.where(here, types_ref[ix, iy, iz : iz + 1], slots - 1).astype(jnp.float32)
                place = [coords_ref[ix, iy, k, iz : iz + 1] for k in range(3)]
                cell = jnp.concatenate(place + [q, kind, jnp.zeros((3, slots), jnp.float32)], axis=0)
                packed_ref[ix, iy, iz] = cell
                for b, at in enumerate((0, cells_z - 1)):
                    if iz == at:
                        faces_ref[ix, iy, b] = cell


def whole_call(kernel, name, outs, operands, smem=0):
    vmem = pl.BlockSpec(memory_space=pltpu.VMEM)
    return pl.pallas_call(
        kernel,
        out_shape=tuple(jax.ShapeDtypeStruct(o, jnp.float32) for o in outs),
        in_specs=[pl.BlockSpec(memory_space=pltpu.SMEM)] * smem + [vmem] * (len(operands) - smem),
        out_specs=(vmem,) * len(outs),
        name=name,
    )(*operands)


def pair_terms(dx, dy, dz, qq, c6, c12, kept=None):
    t = dx * dx + dy * dy + (dz * dz + SOFTEN)
    y = lax.rsqrt(t)
    v = y * y
    v3 = v * v * v
    p = qq * y
    h = c12 * v3
    m = h - c6
    gap = v3 - K3
    u = qq * (y - K1) + gap * m
    z = p + (6.0 * v3) * (m + c12 * gap)
    w = jnp.maximum(EDGE_T - t, 0.0)
    if kept is not None:
        w = jnp.where(kept, w, 0.0)
    return w * ((w * v) * z + 4.0 * u), w * (w * u)


def row_kernel(packed_ref, c6_ref, c12_ref, left_ref, rows_hbm, self_ref, energy_ref, table_ref, rows_ref, sem):
    cells_x, cells_y, cells_z, _, slots = packed_ref.shape
    f32, bf16 = jnp.float32, jnp.bfloat16
    row_id = lax.broadcasted_iota(jnp.int32, (8, slots), 0)
    lane = lax.broadcasted_iota(jnp.int32, (8, slots), 1)
    lane_of = lax.broadcasted_iota(jnp.int32, (cells_z * slots, slots), 1).astype(f32)
    lines = cells_x * cells_y

    kinds = c6_ref.shape[0]
    table_ref[...] = jnp.zeros_like(table_ref)
    c6, c12 = ((0.5 * ENERGY_UNIT) * (c[...] + c[...].T) for c in (c6_ref, c12_ref))
    for k, table in enumerate((c6 - c12 * K3, c12)):
        high = table.astype(bf16)
        at = slice(k * slots, k * slots + kinds)
        table_ref[0:kinds, at] = high
        table_ref[slots : slots + kinds, at] = (table - high.astype(f32)).astype(bf16)

    def store(line):
        slot = line % 2
        return pltpu.make_async_copy(rows_ref.at[slot], rows_hbm.at[line], sem.at[slot])

    def do_line(line, energy):
        ix, iy, slot = line // cells_y, line % cells_y, line % 2

        def placed(iz):
            at = jnp.where(row_id == 0, ix, jnp.where(row_id == 1, iy + 1, jnp.where(row_id == 2, iz + 1, 0)))
            return packed_ref[ix, iy, iz] + at.astype(f32) * CELL_EDGE

        @pl.when(line >= 2)
        def _():
            store(line - 2).wait()

        def split(iz):
            f = placed(iz)
            high = f.astype(bf16).astype(f32)
            mid = (f - high).astype(bf16).astype(f32)
            return jnp.concatenate([high, mid, f - high - mid], axis=0).T.astype(bf16)

        parts = jnp.concatenate([split(iz) for iz in range(cells_z)], axis=0)
        cut = lambda product, k: product[:, k * slots : (k + 1) * slots].reshape(cells_z, slots, slots)
        kinds_of = jnp.dot(parts, left_ref[:, 4 * slots :], preferred_element_type=f32)
        hot = (kinds_of == lane_of).astype(f32).astype(bf16)
        for first in (0, 2):
            mine = jnp.dot(
                parts, left_ref[:, first * slots : (first + 2) * slots], preferred_element_type=f32
            )
            for k in range(2):
                rows_ref[slot, :, first + k] = cut(mine, k)
        looked = jnp.dot(jnp.concatenate([hot, hot], axis=1), table_ref[...], preferred_element_type=f32)
        for k in range(2):
            rows_ref[slot, :, 4 + k] = cut(looked, k)
        store(line).start()

        def inside(iz, energy):
            f = placed(iz)
            bx, by, bz, bq = (jnp.broadcast_to(f[k : k + 1], (8, slots)) for k in range(4))
            kind = jnp.broadcast_to(f[4:5].astype(jnp.int32), (8, slots))
            fold = None
            for at in range(0, slots, 8):
                ax, ay, az, aq, a6, a12 = (rows_ref[slot, iz, k, at : at + 8, :] for k in range(6))
                dx, dy, dz = bx - ax, by - ay, bz - az
                c6, c12 = (
                    jnp.take_along_axis(t, kind, axis=1, mode="promise_in_bounds") for t in (a6, a12)
                )
                s, e = pair_terms(dx, dy, dz, bq * aq, c6, c12, lane != row_id + at)
                energy = energy + e
                moved = (s * dx, s * dy, s * dz)
                fold = moved if fold is None else tuple(a + b for a, b in zip(fold, moved))
            for k in range(3):
                self_ref[line, iz, k] = fold[k]
            return energy

        return lax.fori_loop(0, cells_z, inside, energy)

    energy = lax.fori_loop(0, lines, do_line, jnp.zeros((8, slots), f32))
    energy_ref[...] = 0.5 * energy
    for line in range(max(lines - 2, 0), lines):
        store(line).wait()


def row_call(packed, c6_table, c12_table):
    cells_x, cells_y, cells_z, _, slots = packed.shape
    left = np.zeros((24, 5 * slots), np.float32)
    for k in range(5):
        for n in range(3):
            left[8 * n + k, k * slots : (k + 1) * slots] = 1.0
    left = jnp.asarray(left, jnp.bfloat16)
    atoms = cells_x * cells_y * cells_z * slots
    line = (cells_z, 6, slots, slots)
    vmem = pl.BlockSpec(memory_space=pltpu.VMEM)
    return pl.pallas_call(
        row_kernel,
        out_shape=(
            jax.ShapeDtypeStruct((cells_x * cells_y,) + line, jnp.float32),
            jax.ShapeDtypeStruct((cells_x * cells_y, cells_z, 3, 8, slots), jnp.float32),
            jax.ShapeDtypeStruct((8, slots), jnp.float32),
        ),
        in_specs=[vmem] * 4,
        out_specs=(pl.BlockSpec(memory_space=pl.ANY), vmem, vmem),
        scratch_shapes=[
            pltpu.VMEM((2 * slots, 2 * slots), jnp.bfloat16),
            pltpu.VMEM((2,) + line, jnp.float32),
            pltpu.SemaphoreType.DMA((2,)),
        ],
        cost_estimate=pl.CostEstimate(
            flops=2 * atoms * slots * 376, transcendentals=0, bytes_accessed=atoms * slots * 24
        ),
        name="row_operands",
    )(packed, c6_table, c12_table, left)


def pair_kernel(
    counts_ref, packed_ref, pz_ref, py_ref, px_ref, pc_ref, self_ref, energy_ref, rows_ref,
    own_ref, oz_ref, oy_ref, ozy_ref, ox_ref, fa,
    fe, types, fb, eacc,
):
    cells_x, cells_y, cells_z, _, slots = own_ref.shape
    ext_y, ext_z = cells_y + 2, cells_z + 2
    f32, bf16 = jnp.float32, jnp.bfloat16
    row_id = lax.broadcasted_iota(jnp.int32, (8, slots), 0)
    line = pl.program_id(0)

    @pl.when(line == 0)
    def _():
        eacc[...] = energy_ref[...]

        def place(f, ix, iy, iz):
            at = jnp.where(row_id == 0, ix, jnp.where(row_id == 1, iy, jnp.where(row_id == 2, iz, 0)))
            fe[ix, iy, iz] = f + at.astype(f32) * CELL_EDGE
            types[ix, iy, iz] = f[4:5].astype(jnp.int32)
            fb[ix, iy, iz] = jnp.zeros(fb.shape[3:], f32)

        def place_line(iy, _):
            for ix in range(cells_x):
                for iz in range(cells_z):
                    place(packed_ref[ix, iy, iz], ix, iy + 1, iz + 1)
                    fb[ix, iy + 1, iz + 1] = self_ref[ix * cells_y + iy, iz]
                place(pz_ref[ix, iy, 0], ix, iy + 1, cells_z + 1)
                place(pz_ref[ix, iy, 1], ix, iy + 1, 0)
            for iz in range(ext_z):
                place(px_ref[0, iy, iz], cells_x, iy + 1, iz)
            return 0

        lax.fori_loop(0, cells_y, place_line, 0)
        for iz in range(ext_z):
            for ix in range(cells_x):
                place(py_ref[ix, 0, iz], ix, cells_y + 1, iz)
                fb[ix, 0, iz] = jnp.zeros(fb.shape[3:], f32)
            place(pc_ref[0, 0, iz], cells_x, cells_y + 1, iz)
            place(pc_ref[0, 1, iz], cells_x, 0, iz)

    def row_cell(ix, iy, iz, slot, offsets):
        count = counts_ref[ix, iy, iz]
        quarters = (count + (ROWS // 4 - 1)) // (ROWS // 4)
        full = quarters // 4
        half = (quarters // 2) % 2
        rest = quarters % 2

        def chunk(at, energy, rows):
            at = pl.multiple_of(at, rows)
            here = pl.ds(at, rows)
            ax, ay, az, aq, a6, a12 = (rows_ref[0, slot, k, here, :] for k in range(6))
            fx = fy = fz = None
            for ox, oy, oz in offsets:
                cell = (ix + ox, iy + 1 + oy, iz + 1 + oz)
                spread = lambda k: jnp.broadcast_to(fe[cell[0], cell[1], cell[2], k : k + 1, :], (rows, slots))
                dx = spread(0) - ax
                dy = spread(1) - ay
                dz = spread(2) - az
                qq = spread(3) * aq
                kind = jnp.broadcast_to(types[cell[0], cell[1], cell[2]], (rows, slots))
                c6, c12 = (
                    jnp.take_along_axis(t, kind, axis=1, mode="promise_in_bounds") for t in (a6, a12)
                )
                s, e = pair_terms(dx, dy, dz, qq, c6, c12)
                for r in range(0, rows, 8):
                    energy = energy + e[r : r + 8]
                px, py, pz = s * dx, s * dy, s * dz
                for k, part in enumerate((px, py, pz)):
                    fold = part[0:8]
                    for r in range(8, rows, 8):
                        fold = fold + part[r : r + 8]
                    fb[cell[0], cell[1], cell[2], k] = fb[cell[0], cell[1], cell[2], k] + fold
                if fx is None:
                    fx, fy, fz = px, py, pz
                else:
                    fx, fy, fz = fx + px, fy + py, fz + pz
            for k, part in enumerate((fx, fy, fz)):
                fa[0, slot, k, here, :] = part
            return energy

        energy = lax.fori_loop(0, full, lambda c, e: chunk(c * ROWS, e, ROWS), eacc[...])
        energy = lax.fori_loop(0, half, lambda c, e: chunk(full * ROWS, e, ROWS // 2), energy)
        last = full * ROWS + half * (ROWS // 2)
        eacc[...] = lax.fori_loop(0, rest, lambda c, e: chunk(last, e, ROWS // 4), energy)

    share = rows_ref.shape[1]
    steps = cells_z // share
    ix = line // (cells_y * steps)
    iy = line // steps % cells_y
    low = line % steps * share
    fa[...] = jnp.zeros_like(fa)

    def inner(n, _):
        row_cell(ix, iy, low + n, n, OFFSETS)
        return 0

    lax.fori_loop(0, share, inner, 0)

    @pl.when(line == pl.num_programs(0) - 1)
    def _():
        energy = jnp.sum(eacc[...], axis=0, keepdims=True)

        def total_of(ix, iy, iz):
            parts = [jnp.sum(fb[ix, iy, iz, k], axis=0, keepdims=True) for k in range(3)]
            return jnp.concatenate(parts + [energy, jnp.zeros((4, slots), f32)], axis=0)

        def close_line(iy, _):
            for ix in range(cells_x + 1):
                for iz in range(cells_z):
                    if ix < cells_x:
                        own_ref[ix, iy, iz] = total_of(ix, iy + 1, iz + 1)
                    else:
                        ox_ref[0, iy, iz] = total_of(ix, iy + 1, iz + 1)
                for b, at_z in enumerate((0, cells_z + 1)):
                    oz_ref[ix, iy, b] = total_of(ix, iy + 1, at_z)
            return 0

        lax.fori_loop(0, cells_y, close_line, 0)
        for ix in range(cells_x + 1):
            for a, at_y in enumerate((0, cells_y + 1)):
                for iz in range(cells_z):
                    oy_ref[ix, a, iz] = total_of(ix, at_y, iz + 1)
                for b, at_z in enumerate((0, cells_z + 1)):
                    ozy_ref[ix, a, b] = total_of(ix, at_y, at_z)


def pair_call(counts, pieces, rows, inside, energy):
    cells_x, cells_y, cells_z = counts.shape
    slots = rows.shape[-1]
    f32 = jnp.float32
    fixed = lambda shape: pl.BlockSpec(shape, lambda i: (0,) * len(shape))
    outs = [
        dims + (8, slots)
        for dims in (
            (cells_x, cells_y, cells_z),
            (cells_x + 1, cells_y, 2),
            (cells_x + 1, 2, cells_z),
            (cells_x + 1, 2, 2),
            (1, cells_y, cells_z),
        )
    ]
    steps = 2 if cells_z % 2 == 0 else 1
    lines = cells_x * cells_y
    rows = rows.reshape((lines * steps, cells_z // steps) + rows.shape[2:])
    sums = rows.shape[:2] + (3, slots, slots)
    by_line = lambda shape: pl.BlockSpec((1,) + shape[1:], lambda i: (i, 0, 0, 0, 0))
    grown = (cells_x + 1, cells_y + 2, cells_z + 2)
    *outs, sums = pl.pallas_call(
        pair_kernel,
        grid=(lines * steps,),
        out_shape=tuple(jax.ShapeDtypeStruct(o, f32) for o in outs + [sums]),
        in_specs=[pl.BlockSpec(memory_space=pltpu.SMEM)]
        + [fixed(piece.shape) for piece in (*pieces, inside, energy)]
        + [by_line(rows.shape)],
        out_specs=tuple(fixed(o) for o in outs) + (by_line(sums),),
        scratch_shapes=[
            pltpu.VMEM(grown + (8, slots), f32),
            pltpu.VMEM(grown + (1, slots), jnp.int32),
            pltpu.VMEM(grown + (3, 8, slots), f32),
            pltpu.VMEM((8, slots), f32),
        ],
        name="pair_forces",
    )(counts, *pieces, inside, energy, rows)
    return (*outs, sums.reshape((lines, cells_z) + sums.shape[2:]))


def own_kernel(sums_ref, own_ref, ends_ref, out_ref):
    f32, bf16 = jnp.float32, jnp.bfloat16
    for iz in range(sums_ref.shape[1]):
        halves = []
        for k in range(3):
            whole = sums_ref[0, iz, k]
            high = whole.astype(bf16)
            halves += [high, (whole - high.astype(f32)).astype(bf16)]
        total = jnp.dot(jnp.concatenate(halves, axis=1), ends_ref[...], preferred_element_type=f32)
        out_ref[0, iz] = own_ref[0, iz] - total.T[:8]


def own_call(sums, own, low, high):
    cells_x, cells_y, cells_z, _, slots = own.shape
    ends = np.zeros((6 * slots, slots), np.float32)
    for k in range(3):
        ends[2 * k * slots : 2 * (k + 1) * slots, k] = 1.0
    ends = jnp.asarray(ends, jnp.bfloat16)
    block = (1, cells_z, 8, slots)
    share = sums.size // sums.shape[0] * (high - low)
    return pl.pallas_call(
        own_kernel,
        grid=(high - low,),
        out_shape=jax.ShapeDtypeStruct((high - low,) + block[1:], jnp.float32),
        in_specs=[
            pl.BlockSpec((1,) + sums.shape[1:], lambda i: (i + low, 0, 0, 0, 0)),
            pl.BlockSpec(block, lambda i: (i + low, 0, 0, 0)),
            pl.BlockSpec(ends.shape, lambda i: (0, 0)),
        ],
        out_specs=pl.BlockSpec(block, lambda i: (i, 0, 0, 0)),
        cost_estimate=pl.CostEstimate(flops=8 * share, transcendentals=0, bytes_accessed=4 * share),
        name="own_rows",
    )(sums, own.reshape((-1,) + block[1:]), ends)


def final_kernel(front_ref, back_ref, rz_ref, ry_ref, rzy_ref, rx_ref, *refs):
    *terms, forces_ref, energy_ref = refs
    cells_x, cells_y, _, cells_z, slots = forces_ref.shape
    split = front_ref.shape[0]
    for ix in range(cells_x):
        for iy in range(cells_y):
            sides_y = [m for m, at in enumerate((cells_y - 1, 0)) if iy == at]
            for iz in range(cells_z):
                sides_z = [n for n, at in enumerate((cells_z - 1, 0)) if iz == at]
                line = ix * cells_y + iy
                f = front_ref[line, iz] if line < split else back_ref[line - split, iz]
                for n in sides_z:
                    f = f + rz_ref[ix, iy, n]
                for m in sides_y:
                    f = f + ry_ref[ix, m, iz]
                    for n in sides_z:
                        f = f + rzy_ref[ix, m, n]
                if ix == 0:
                    f = f + rx_ref[0, iy, iz]
                if ix == 0 and iy == 0 and iz == 0:
                    energy = f[3:4]
                for k in range(3):
                    forces_ref[ix, iy, k, iz : iz + 1] = f[k : k + 1]
    for term in terms:
        energy = energy + term[...]
    energy_ref[...] = jnp.broadcast_to(jnp.sum(energy, axis=1, keepdims=True), (1, slots))


def both_ways(block, dim, step, size):
    if size == 2:
        return moved(block, *step)
    down = moved(lax.slice_in_dim(block, 0, 1, axis=dim), *(-d for d in step))
    up = moved(lax.slice_in_dim(block, 1, 2, axis=dim), *step)
    return jnp.concatenate([down, up], axis=dim)


def to_sides(z, y, zy, ny, nz):
    if ny == 2 and nz == 2:
        corners = moved(zy, 0, 1, 1)
    else:
        corners = jnp.concatenate(
            [
                jnp.concatenate(
                    [moved(zy[:, a : a + 1, b : b + 1], 0, 2 * a - 1, 2 * b - 1) for b in range(2)], axis=2
                )
                for a in range(2)
            ],
            axis=1,
        )
    return both_ways(z, 2, (0, 0, 1), nz), both_ways(y, 1, (0, 1, 0), ny), corners


def spread(block, dim, size):
    zeros = jnp.zeros(block.shape[:dim] + (size - 2,) + block.shape[dim + 1 :], block.dtype)
    down, up = (lax.slice_in_dim(block, m, m + 1, axis=dim) for m in range(2))
    return jnp.concatenate([up, zeros, down], axis=dim)


def on_device(coords, charges, atom_types, counts, c6_table, c12_table):
    slots = coords.shape[-1]
    cells_x, cells_y, cells_z = coords.shape[:3]
    nx, ny, nz = (lax.axis_size(a) for a in AXES)
    tail = (8, slots)
    packed, faces = whole_call(
        pack_kernel,
        "pack_cells",
        [(cells_x, cells_y, cells_z) + tail, (cells_x, cells_y, 2) + tail],
        (counts, jnp.swapaxes(coords, 2, 3), charges, atom_types),
        smem=1,
    )
    pz = both_ways(faces, 2, (0, 0, 1), nz)
    lines = jnp.concatenate([pz[:, :, 1:], packed, pz[:, :, :1]], axis=2)
    ends = jnp.concatenate([lines[:1, :1], lines[:1, cells_y - 1 :]], axis=1)
    px = moved(lines[:1], -1, 0, 0)
    py = moved(lines[:, :1], 0, -1, 0)
    if ny == 2:
        pc = moved(ends, -1, -1, 0)
    else:
        pc = jnp.concatenate([moved(ends[:, :1], -1, -1, 0), moved(ends[:, 1:], -1, 1, 0)], axis=1)
    rows, inside, within = row_call(packed, c6_table, c12_table)
    own, oz, oy, ozy, ox, sums = pair_call(
        counts, (packed, pz, py, px, pc), rows, inside, within
    )
    rz, ry, rzy = to_sides(oz, oy, ozy, ny, nz)
    lines = cells_x * cells_y
    split = (lines + 1) // 2
    front, rz = lax.optimization_barrier((own_call(sums, own, 0, split), rz))
    ox = (
        ox
        + spread(rz[cells_x:], 2, cells_z)
        + spread(ry[cells_x:], 1, cells_y)
        + spread(spread(rzy[cells_x:], 2, cells_z), 1, cells_y)
    )
    rx = moved(ox, 1, 0, 0)
    sums, ox = lax.optimization_barrier((sums, ox))
    back = own_call(sums, own, split, lines)
    if nz == 2 and ny == 2 and 2 <= nx <= 4:
        summed = ox[0, 0, 0, 3:4]
        terms = [moved(summed, i, 0, 0) for i in range(2, nx)]
    else:
        terms = [lax.psum(own[0, 0, 0, 3:4], AXES)]
        rz, ry, rzy, rx = (r.at[..., 3, :].set(0.0) for r in (rz, ry, rzy, rx))
        front = front.at[..., 3, :].set(0.0)
    forces, energy = whole_call(
        final_kernel,
        "join_forces",
        [(cells_x, cells_y, 3, cells_z, slots), (1, slots)],
        (front, back, rz, ry, rzy, rx, *terms),
    )
    return (jnp.swapaxes(forces, 2, 3), energy[0, :1])


def solution(mesh):
    return jax.shard_map(
        on_device,
        mesh=mesh,
        in_specs=(
            P(("groups", "gx"), "gy", "gz", None, None),
            P(("groups", "gx"), "gy", "gz", None),
            P(("groups", "gx"), "gy", "gz", None),
            P(("groups", "gx"), "gy", "gz"),
            P(),
            P(),
        ),
        out_specs=(P(("groups", "gx"), "gy", "gz", None, None), P("groups")),
        check_vma=False,
    )
```

```python
import jax
import jax.numpy as jnp
import numpy as np
from jax import lax
from jax.experimental import pallas as pl
from jax.experimental.pallas import tpu as pltpu
from jax.sharding import PartitionSpec as P

CELL_EDGE = 1.1
CUT_SQUARE = 1.0
SOFTEN = 0.09
ENERGY_UNIT = 0.1
EDGE_T = CUT_SQUARE + SOFTEN
K1 = EDGE_T**-0.5
K3 = EDGE_T**-3.0
K6 = EDGE_T**-6.0
OFFSETS = (
    (0, 0, 1),
    (0, 1, 0),
    (0, 1, 1),
    (0, 1, -1),
) + tuple((1, oy, oz) for oy in (-1, 0, 1) for oz in (-1, 0, 1))
ROWS = 32
AXES = ("gx", "gy", "gz")


def moved(block, dx, dy, dz):
    nx, ny, nz = (lax.axis_size(a) for a in AXES)
    flat = lambda i, j, k: ((i % nx) * ny + j % ny) * nz + k % nz
    cells = [(i, j, k) for i in range(nx) for j in range(ny) for k in range(nz)]
    route = [(flat(i - dx, j - dy, k - dz), flat(i, j, k)) for i, j, k in cells]
    return lax.ppermute(block, AXES, route)


def pack_kernel(counts_ref, coords_ref, charges_ref, types_ref, packed_ref, faces_ref):
    cells_x, cells_y, _, cells_z, slots = coords_ref.shape
    lane = lax.broadcasted_iota(jnp.int32, (1, slots), 1)
    for ix in range(cells_x):
        for iy in range(cells_y):
            for iz in range(cells_z):
                here = lane < counts_ref[ix, iy, iz]
                q = jnp.where(here, charges_ref[ix, iy, iz : iz + 1] * ENERGY_UNIT**0.5, 0.0)
                kind = jnp.where(here, types_ref[ix, iy, iz : iz + 1], slots - 1).astype(jnp.float32)
                place = [coords_ref[ix, iy, k, iz : iz + 1] for k in range(3)]
                cell = jnp.concatenate(place + [q, kind, jnp.zeros((3, slots), jnp.float32)], axis=0)
                packed_ref[ix, iy, iz] = cell
                for b, at in enumerate((0, cells_z - 1)):
                    if iz == at:
                        faces_ref[ix, iy, b] = cell


def whole_call(kernel, name, outs, operands, smem=0):
    vmem = pl.BlockSpec(memory_space=pltpu.VMEM)
    return pl.pallas_call(
        kernel,
        out_shape=tuple(jax.ShapeDtypeStruct(o, jnp.float32) for o in outs),
        in_specs=[pl.BlockSpec(memory_space=pltpu.SMEM)] * smem + [vmem] * (len(operands) - smem),
        out_specs=(vmem,) * len(outs),
        name=name,
    )(*operands)


def pair_terms(dx, dy, dz, qq, c6, c12, kept=None):
    t = dx * dx + dy * dy + (dz * dz + SOFTEN)
    y = lax.rsqrt(t)
    v = y * y
    v3 = v * v * v
    p = qq * y
    h = c12 * v3
    m = h - c6
    gap = v3 - K3
    u = qq * (y - K1) + gap * m
    z = p + (6.0 * v3) * (m + c12 * gap)
    w = jnp.maximum(EDGE_T - t, 0.0)
    if kept is not None:
        w = jnp.where(kept, w, 0.0)
    return w * ((w * v) * z + 4.0 * u), w * (w * u)


def row_kernel(packed_ref, c6_ref, c12_ref, left_ref, rows_hbm, self_ref, energy_ref, table_ref, rows_ref, sem):
    cells_x, cells_y, cells_z, _, slots = packed_ref.shape
    f32, bf16 = jnp.float32, jnp.bfloat16
    row_id = lax.broadcasted_iota(jnp.int32, (8, slots), 0)
    lane = lax.broadcasted_iota(jnp.int32, (8, slots), 1)
    lane_of = lax.broadcasted_iota(jnp.int32, (cells_z * slots, slots), 1).astype(f32)
    lines = cells_x * cells_y

    kinds = c6_ref.shape[0]
    table_ref[...] = jnp.zeros_like(table_ref)
    c6, c12 = ((0.5 * ENERGY_UNIT) * (c[...] + c[...].T) for c in (c6_ref, c12_ref))
    for k, table in enumerate((c6 - c12 * K3, c12)):
        high = table.astype(bf16)
        at = slice(k * slots, k * slots + kinds)
        table_ref[0:kinds, at] = high
        table_ref[slots : slots + kinds, at] = (table - high.astype(f32)).astype(bf16)

    def store(line):
        slot = line % 2
        return pltpu.make_async_copy(rows_ref.at[slot], rows_hbm.at[line], sem.at[slot])

    def do_line(line, energy):
        ix, iy, slot = line // cells_y, line % cells_y, line % 2

        def placed(iz):
            at = jnp.where(row_id == 0, ix, jnp.where(row_id == 1, iy + 1, jnp.where(row_id == 2, iz + 1, 0)))
            return packed_ref[ix, iy, iz] + at.astype(f32) * CELL_EDGE

        @pl.when(line >= 2)
        def _():
            store(line - 2).wait()

        def split(iz):
            f = placed(iz)
            high = f.astype(bf16).astype(f32)
            mid = (f - high).astype(bf16).astype(f32)
            return jnp.concatenate([high, mid, f - high - mid], axis=0).T.astype(bf16)

        parts = jnp.concatenate([split(iz) for iz in range(cells_z)], axis=0)
        cut = lambda product, k: product[:, k * slots : (k + 1) * slots].reshape(cells_z, slots, slots)
        kinds_of = jnp.dot(parts, left_ref[:, 4 * slots :], preferred_element_type=f32)
        hot = (kinds_of == lane_of).astype(f32).astype(bf16)
        for first in (0, 2):
            mine = jnp.dot(
                parts, left_ref[:, first * slots : (first + 2) * slots], preferred_element_type=f32
            )
            for k in range(2):
                rows_ref[slot, :, first + k] = cut(mine, k)
        looked = jnp.dot(jnp.concatenate([hot, hot], axis=1), table_ref[...], preferred_element_type=f32)
        for k in range(2):
            rows_ref[slot, :, 4 + k] = cut(looked, k)
        store(line).start()

        def inside(iz, energy):
            f = placed(iz)
            bx, by, bz, bq = (jnp.broadcast_to(f[k : k + 1], (8, slots)) for k in range(4))
            kind = jnp.broadcast_to(f[4:5].astype(jnp.int32), (8, slots))
            fold = None
            for at in range(0, slots, 8):
                ax, ay, az, aq, a6, a12 = (rows_ref[slot, iz, k, at : at + 8, :] for k in range(6))
                dx, dy, dz = bx - ax, by - ay, bz - az
                c6, c12 = (
                    jnp.take_along_axis(t, kind, axis=1, mode="promise_in_bounds") for t in (a6, a12)
                )
                s, e = pair_terms(dx, dy, dz, bq * aq, c6, c12, lane != row_id + at)
                energy = energy + e
                moved = (s * dx, s * dy, s * dz)
                fold = moved if fold is None else tuple(a + b for a, b in zip(fold, moved))
            for k in range(3):
                self_ref[line, iz, k] = fold[k]
            return energy

        return lax.fori_loop(0, cells_z, inside, energy, unroll=2 if cells_z % 2 == 0 else 1)

    energy = lax.fori_loop(0, lines, do_line, jnp.zeros((8, slots), f32))
    energy_ref[...] = 0.5 * energy
    for line in range(max(lines - 2, 0), lines):
        store(line).wait()


def row_call(packed, c6_table, c12_table):
    cells_x, cells_y, cells_z, _, slots = packed.shape
    left = np.zeros((24, 5 * slots), np.float32)
    for k in range(5):
        for n in range(3):
            left[8 * n + k, k * slots : (k + 1) * slots] = 1.0
    left = jnp.asarray(left, jnp.bfloat16)
    atoms = cells_x * cells_y * cells_z * slots
    line = (cells_z, 6, slots, slots)
    vmem = pl.BlockSpec(memory_space=pltpu.VMEM)
    return pl.pallas_call(
        row_kernel,
        out_shape=(
            jax.ShapeDtypeStruct((cells_x * cells_y,) + line, jnp.float32),
            jax.ShapeDtypeStruct((cells_x * cells_y, cells_z, 3, 8, slots), jnp.float32),
            jax.ShapeDtypeStruct((8, slots), jnp.float32),
        ),
        in_specs=[vmem] * 4,
        out_specs=(pl.BlockSpec(memory_space=pl.ANY), vmem, vmem),
        scratch_shapes=[
            pltpu.VMEM((2 * slots, 2 * slots), jnp.bfloat16),
            pltpu.VMEM((2,) + line, jnp.float32),
            pltpu.SemaphoreType.DMA((2,)),
        ],
        cost_estimate=pl.CostEstimate(
            flops=2 * atoms * slots * 376, transcendentals=0, bytes_accessed=atoms * slots * 24
        ),
        name="row_operands",
    )(packed, c6_table, c12_table, left)


def pair_kernel(
    counts_ref, packed_ref, pz_ref, py_ref, px_ref, pc_ref, self_ref, energy_ref, rows_ref,
    own_ref, oz_ref, oy_ref, ozy_ref, ox_ref, fa,
    fe, types, fb, eacc,
):
    cells_x, cells_y, cells_z, _, slots = own_ref.shape
    ext_y, ext_z = cells_y + 2, cells_z + 2
    f32, bf16 = jnp.float32, jnp.bfloat16
    row_id = lax.broadcasted_iota(jnp.int32, (8, slots), 0)
    line = pl.program_id(0)

    @pl.when(line == 0)
    def _():
        eacc[...] = energy_ref[...]

        def place(f, ix, iy, iz):
            at = jnp.where(row_id == 0, ix, jnp.where(row_id == 1, iy, jnp.where(row_id == 2, iz, 0)))
            fe[ix, iy, iz] = f + at.astype(f32) * CELL_EDGE
            types[ix, iy, iz] = f[4:5].astype(jnp.int32)
            fb[ix, iy, iz] = jnp.zeros(fb.shape[3:], f32)

        def place_line(iy, _):
            for ix in range(cells_x):
                for iz in range(cells_z):
                    place(packed_ref[ix, iy, iz], ix, iy + 1, iz + 1)
                    fb[ix, iy + 1, iz + 1] = self_ref[ix * cells_y + iy, iz]
                place(pz_ref[ix, iy, 0], ix, iy + 1, cells_z + 1)
                place(pz_ref[ix, iy, 1], ix, iy + 1, 0)
            for iz in range(ext_z):
                place(px_ref[0, iy, iz], cells_x, iy + 1, iz)
            return 0

        lax.fori_loop(0, cells_y, place_line, 0)
        for iz in range(ext_z):
            for ix in range(cells_x):
                place(py_ref[ix, 0, iz], ix, cells_y + 1, iz)
                fb[ix, 0, iz] = jnp.zeros(fb.shape[3:], f32)
            place(pc_ref[0, 0, iz], cells_x, cells_y + 1, iz)
            place(pc_ref[0, 1, iz], cells_x, 0, iz)

    def row_cell(ix, iy, iz, slot, offsets):
        count = counts_ref[ix, iy, iz]
        quarters = (count + (ROWS // 4 - 1)) // (ROWS // 4)
        full = quarters // 4
        half = (quarters // 2) % 2
        rest = quarters % 2

        def chunk(at, energy, rows):
            at = pl.multiple_of(at, rows)
            here = pl.ds(at, rows)
            ax, ay, az, aq, a6, a12 = (rows_ref[0, slot, k, here, :] for k in range(6))
            fx = fy = fz = None
            for ox, oy, oz in offsets:
                cell = (ix + ox, iy + 1 + oy, iz + 1 + oz)
                spread = lambda k: jnp.broadcast_to(fe[cell[0], cell[1], cell[2], k : k + 1, :], (rows, slots))
                dx = spread(0) - ax
                dy = spread(1) - ay
                dz = spread(2) - az
                qq = spread(3) * aq
                kind = jnp.broadcast_to(types[cell[0], cell[1], cell[2]], (rows, slots))
                c6, c12 = (
                    jnp.take_along_axis(t, kind, axis=1, mode="promise_in_bounds") for t in (a6, a12)
                )
                s, e = pair_terms(dx, dy, dz, qq, c6, c12)
                for r in range(0, rows, 8):
                    energy = energy + e[r : r + 8]
                px, py, pz = s * dx, s * dy, s * dz
                for k, part in enumerate((px, py, pz)):
                    fold = part[0:8]
                    for r in range(8, rows, 8):
                        fold = fold + part[r : r + 8]
                    fb[cell[0], cell[1], cell[2], k] = fb[cell[0], cell[1], cell[2], k] + fold
                if fx is None:
                    fx, fy, fz = px, py, pz
                else:
                    fx, fy, fz = fx + px, fy + py, fz + pz
            for k, part in enumerate((fx, fy, fz)):
                fa[0, slot, k, here, :] = part
            return energy

        energy = lax.fori_loop(0, full, lambda c, e: chunk(c * ROWS, e, ROWS), eacc[...])
        energy = lax.fori_loop(0, half, lambda c, e: chunk(full * ROWS, e, ROWS // 2), energy)
        last = full * ROWS + half * (ROWS // 2)
        eacc[...] = lax.fori_loop(0, rest, lambda c, e: chunk(last, e, ROWS // 4), energy)

    share = rows_ref.shape[1]
    steps = cells_z // share
    ix = line // (cells_y * steps)
    iy = line // steps % cells_y
    low = line % steps * share
    fa[...] = jnp.zeros_like(fa)

    def inner(n, _):
        row_cell(ix, iy, low + n, n, OFFSETS)
        return 0

    lax.fori_loop(0, share, inner, 0)

    @pl.when(line == pl.num_programs(0) - 1)
    def _():
        energy = jnp.sum(eacc[...], axis=0, keepdims=True)

        def total_of(ix, iy, iz):
            parts = [jnp.sum(fb[ix, iy, iz, k], axis=0, keepdims=True) for k in range(3)]
            return jnp.concatenate(parts + [energy, jnp.zeros((4, slots), f32)], axis=0)

        def close_line(iy, _):
            for ix in range(cells_x + 1):
                for iz in range(cells_z):
                    if ix < cells_x:
                        own_ref[ix, iy, iz] = total_of(ix, iy + 1, iz + 1)
                    else:
                        ox_ref[0, iy, iz] = total_of(ix, iy + 1, iz + 1)
                for b, at_z in enumerate((0, cells_z + 1)):
                    oz_ref[ix, iy, b] = total_of(ix, iy + 1, at_z)
            return 0

        lax.fori_loop(0, cells_y, close_line, 0)
        for ix in range(cells_x + 1):
            for a, at_y in enumerate((0, cells_y + 1)):
                for iz in range(cells_z):
                    oy_ref[ix, a, iz] = total_of(ix, at_y, iz + 1)
                for b, at_z in enumerate((0, cells_z + 1)):
                    ozy_ref[ix, a, b] = total_of(ix, at_y, at_z)


def pair_call(counts, pieces, rows, inside, energy):
    cells_x, cells_y, cells_z = counts.shape
    slots = rows.shape[-1]
    f32 = jnp.float32
    fixed = lambda shape: pl.BlockSpec(shape, lambda i: (0,) * len(shape))
    outs = [
        dims + (8, slots)
        for dims in (
            (cells_x, cells_y, cells_z),
            (cells_x + 1, cells_y, 2),
            (cells_x + 1, 2, cells_z),
            (cells_x + 1, 2, 2),
            (1, cells_y, cells_z),
        )
    ]
    steps = 2 if cells_z % 2 == 0 else 1
    lines = cells_x * cells_y
    rows = rows.reshape((lines * steps, cells_z // steps) + rows.shape[2:])
    sums = rows.shape[:2] + (3, slots, slots)
    by_line = lambda shape: pl.BlockSpec((1,) + shape[1:], lambda i: (i, 0, 0, 0, 0))
    grown = (cells_x + 1, cells_y + 2, cells_z + 2)
    *outs, sums = pl.pallas_call(
        pair_kernel,
        grid=(lines * steps,),
        out_shape=tuple(jax.ShapeDtypeStruct(o, f32) for o in outs + [sums]),
        in_specs=[pl.BlockSpec(memory_space=pltpu.SMEM)]
        + [fixed(piece.shape) for piece in (*pieces, inside, energy)]
        + [by_line(rows.shape)],
        out_specs=tuple(fixed(o) for o in outs) + (by_line(sums),),
        scratch_shapes=[
            pltpu.VMEM(grown + (8, slots), f32),
            pltpu.VMEM(grown + (1, slots), jnp.int32),
            pltpu.VMEM(grown + (3, 8, slots), f32),
            pltpu.VMEM((8, slots), f32),
        ],
        name="pair_forces",
    )(counts, *pieces, inside, energy, rows)
    return (*outs, sums.reshape((lines, cells_z) + sums.shape[2:]))


def own_kernel(sums_ref, own_ref, ends_ref, out_ref):
    f32, bf16 = jnp.float32, jnp.bfloat16
    for iz in range(sums_ref.shape[1]):
        halves = []
        for k in range(3):
            whole = sums_ref[0, iz, k]
            high = whole.astype(bf16)
            halves += [high, (whole - high.astype(f32)).astype(bf16)]
        total = jnp.dot(jnp.concatenate(halves, axis=1), ends_ref[...], preferred_element_type=f32)
        out_ref[0, iz] = own_ref[0, iz] - total.T[:8]


def own_call(sums, own, low, high):
    cells_x, cells_y, cells_z, _, slots = own.shape
    ends = np.zeros((6 * slots, slots), np.float32)
    for k in range(3):
        ends[2 * k * slots : 2 * (k + 1) * slots, k] = 1.0
    ends = jnp.asarray(ends, jnp.bfloat16)
    block = (1, cells_z, 8, slots)
    share = sums.size // sums.shape[0] * (high - low)
    return pl.pallas_call(
        own_kernel,
        grid=(high - low,),
        out_shape=jax.ShapeDtypeStruct((high - low,) + block[1:], jnp.float32),
        in_specs=[
            pl.BlockSpec((1,) + sums.shape[1:], lambda i: (i + low, 0, 0, 0, 0)),
            pl.BlockSpec(block, lambda i: (i + low, 0, 0, 0)),
            pl.BlockSpec(ends.shape, lambda i: (0, 0)),
        ],
        out_specs=pl.BlockSpec(block, lambda i: (i, 0, 0, 0)),
        cost_estimate=pl.CostEstimate(flops=8 * share, transcendentals=0, bytes_accessed=4 * share),
        name="own_rows",
    )(sums, own.reshape((-1,) + block[1:]), ends)


def final_kernel(front_ref, back_ref, rz_ref, ry_ref, rzy_ref, rx_ref, *refs):
    *terms, forces_ref, energy_ref = refs
    cells_x, cells_y, _, cells_z, slots = forces_ref.shape
    split = front_ref.shape[0]
    for ix in range(cells_x):
        for iy in range(cells_y):
            sides_y = [m for m, at in enumerate((cells_y - 1, 0)) if iy == at]
            for iz in range(cells_z):
                sides_z = [n for n, at in enumerate((cells_z - 1, 0)) if iz == at]
                line = ix * cells_y + iy
                f = front_ref[line, iz] if line < split else back_ref[line - split, iz]
                for n in sides_z:
                    f = f + rz_ref[ix, iy, n]
                for m in sides_y:
                    f = f + ry_ref[ix, m, iz]
                    for n in sides_z:
                        f = f + rzy_ref[ix, m, n]
                if ix == 0:
                    f = f + rx_ref[0, iy, iz]
                if ix == 0 and iy == 0 and iz == 0:
                    energy = f[3:4]
                for k in range(3):
                    forces_ref[ix, iy, k, iz : iz + 1] = f[k : k + 1]
    for term in terms:
        energy = energy + term[...]
    energy_ref[...] = jnp.broadcast_to(jnp.sum(energy, axis=1, keepdims=True), (1, slots))


def both_ways(block, dim, step, size):
    if size == 2:
        return moved(block, *step)
    down = moved(lax.slice_in_dim(block, 0, 1, axis=dim), *(-d for d in step))
    up = moved(lax.slice_in_dim(block, 1, 2, axis=dim), *step)
    return jnp.concatenate([down, up], axis=dim)


def to_sides(z, y, zy, ny, nz):
    if ny == 2 and nz == 2:
        corners = moved(zy, 0, 1, 1)
    else:
        corners = jnp.concatenate(
            [
                jnp.concatenate(
                    [moved(zy[:, a : a + 1, b : b + 1], 0, 2 * a - 1, 2 * b - 1) for b in range(2)], axis=2
                )
                for a in range(2)
            ],
            axis=1,
        )
    return both_ways(z, 2, (0, 0, 1), nz), both_ways(y, 1, (0, 1, 0), ny), corners


def spread(block, dim, size):
    zeros = jnp.zeros(block.shape[:dim] + (size - 2,) + block.shape[dim + 1 :], block.dtype)
    down, up = (lax.slice_in_dim(block, m, m + 1, axis=dim) for m in range(2))
    return jnp.concatenate([up, zeros, down], axis=dim)


def on_device(coords, charges, atom_types, counts, c6_table, c12_table):
    slots = coords.shape[-1]
    cells_x, cells_y, cells_z = coords.shape[:3]
    nx, ny, nz = (lax.axis_size(a) for a in AXES)
    tail = (8, slots)
    packed, faces = whole_call(
        pack_kernel,
        "pack_cells",
        [(cells_x, cells_y, cells_z) + tail, (cells_x, cells_y, 2) + tail],
        (counts, jnp.swapaxes(coords, 2, 3), charges, atom_types),
        smem=1,
    )
    pz = both_ways(faces, 2, (0, 0, 1), nz)
    lines = jnp.concatenate([pz[:, :, 1:], packed, pz[:, :, :1]], axis=2)
    ends = jnp.concatenate([lines[:1, :1], lines[:1, cells_y - 1 :]], axis=1)
    px = moved(lines[:1], -1, 0, 0)
    py = moved(lines[:, :1], 0, -1, 0)
    if ny == 2:
        pc = moved(ends, -1, -1, 0)
    else:
        pc = jnp.concatenate([moved(ends[:, :1], -1, -1, 0), moved(ends[:, 1:], -1, 1, 0)], axis=1)
    rows, inside, within = row_call(packed, c6_table, c12_table)
    own, oz, oy, ozy, ox, sums = pair_call(
        counts, (packed, pz, py, px, pc), rows, inside, within
    )
    rz, ry, rzy = to_sides(oz, oy, ozy, ny, nz)
    lines = cells_x * cells_y
    split = (lines + 1) // 2
    front, rz = lax.optimization_barrier((own_call(sums, own, 0, split), rz))
    ox = (
        ox
        + spread(rz[cells_x:], 2, cells_z)
        + spread(ry[cells_x:], 1, cells_y)
        + spread(spread(rzy[cells_x:], 2, cells_z), 1, cells_y)
    )
    rx = moved(ox, 1, 0, 0)
    sums, ox = lax.optimization_barrier((sums, ox))
    back = own_call(sums, own, split, lines)
    if nz == 2 and ny == 2 and 2 <= nx <= 4:
        summed = ox[0, 0, 0, 3:4]
        terms = [moved(summed, i, 0, 0) for i in range(2, nx)]
    else:
        terms = [lax.psum(own[0, 0, 0, 3:4], AXES)]
        rz, ry, rzy, rx = (r.at[..., 3, :].set(0.0) for r in (rz, ry, rzy, rx))
        front = front.at[..., 3, :].set(0.0)
    forces, energy = whole_call(
        final_kernel,
        "join_forces",
        [(cells_x, cells_y, 3, cells_z, slots), (1, slots)],
        (front, back, rz, ry, rzy, rx, *terms),
    )
    return (jnp.swapaxes(forces, 2, 3), energy[0, :1])


def solution(mesh):
    return jax.shard_map(
        on_device,
        mesh=mesh,
        in_specs=(
            P(("groups", "gx"), "gy", "gz", None, None),
            P(("groups", "gx"), "gy", "gz", None),
            P(("groups", "gx"), "gy", "gz", None),
            P(("groups", "gx"), "gy", "gz"),
            P(),
            P(),
        ),
        out_specs=(P(("groups", "gx"), "gy", "gz", None, None), P("groups")),
        check_vma=False,
    )
```
